256 devices in a mesh: fft: 32 (over x_lo, z, core), scal: 8 (over x_hi, y).
Axes of the slice: x: 4 (x_hi: 2, x_lo: 2; x = x_hi * 2 + x_lo), y: 4, z: 8, core: 2. Of those that a mesh axis runs over, the one named last changes fastest.
Arguments:
- scalar_state: float32 [8, 2, 256, 256, 128], P('scal', None, 'fft'), may hold values from -12 to 12
- velocity: bfloat16 [3, 256, 256, 256], P(None, 'fft', 'scal'), may hold values from -6 to 6
- species: int32 [8], P('scal'), may hold values from 0 to 63
- kappa_table: float32 [64], replicated, may hold values from 0.1 to 1
- dealias_bound: int32 [8], P('scal'), may hold values from 64 to 85
Outputs:
- new_state: float32 [8, 2, 256, 256, 128], P('scal', None, 'fft')
- kappa: float32 [8], P('scal')
The draws below stay inside these ranges and needn't reach their ends.
All inputs are finite; a program needn't handle non-finite values.
Results may differ from the reference program's by a relative error of at most 0.0027.
Values may be sent and summed in bfloat16 or wider, within the bound.
A program may use at most 128 MiB of HBM per device.

```python
import math
import jax
import jax.numpy as jnp
from jax import lax

N = 256
SPECIES = 64
SCALARS = 8


def draw_scalar_state(key, part):
    dims_shape = (SCALARS, 2, N, N, N // 2)
    key_base, key_rough, key_scale = jax.random.split(key, 3)
    values = jnp.clip(jax.random.normal(key_base, dims_shape, jnp.float32), -4.0, 4.0)
    roughness = jnp.exp(jax.random.uniform(key_rough, dims_shape, jnp.float32, math.log(0.5), math.log(1.5)))
    ky_float = jnp.arange(N, dtype=jnp.int32).astype(jnp.float32)
    envelope = jnp.sqrt(1.0 + 2.0 * ky_float / (N - 1)).reshape(1, 1, N, 1, 1)
    scalar_scale = jnp.exp(jax.random.uniform(key_scale, (SCALARS, 1, 1, 1, 1), jnp.float32, math.log(0.5), math.log(2.0)))
    return jnp.clip(values * roughness * envelope * scalar_scale, -12.0, 12.0).astype(jnp.float32)


def plant(result, rng, low, largest):
    longest = result.shape.index(max(result.shape))
    spots = []
    for shift in (0, 1):
        where = [jax.random.randint(jax.random.fold_in(rng, axis), (), 0, length) for axis, length in enumerate(result.shape)]
        where[longest] = (where[longest] + shift) % result.shape[longest]
        spots.append(tuple(where))
    return result.at[spots[0]].set(low).at[spots[1]].set(largest)


def steps_of(rng, extent, pieces, least, high):
    loudness, own = 1.0, jax.random.fold_in(rng, 6)
    for position, parts in pieces:
        draws = jnp.exp(jax.random.uniform(jax.random.fold_in(own, position), (parts,), jnp.float32, least / len(pieces), high / len(pieces)))
        loudness = loudness * jnp.repeat(draws, extent[position] // parts).reshape([-1 if axis == position else 1 for axis in range(len(extent))])
    return loudness


def normal_values(key, dims, spread, most, cuts=(), held_as=jnp.bfloat16):
    drawn = jax.random.normal(key, dims, jnp.float32) * spread
    if len(cuts) > 0:
        drawn = steps_of(key, dims, cuts, -0.22, 0.18) * drawn
    return jnp.clip(drawn, min=-most, max=most).astype(held_as)


def setup_inputs(seed: int = 0) -> dict:
    keys = jax.random.split(jax.random.key(seed), 6)
    return {
        "scalar_state": draw_scalar_state(jax.random.fold_in(keys[5], 71), 0),
        "velocity": normal_values(keys[1], (3, N, N, N), 1.0, 6.0, ((1, 32), (2, 8))),
        "species": plant(jax.random.randint(keys[2], (SCALARS,), 0, SPECIES), jax.random.fold_in(keys[2], 1), 0, SPECIES - 1).astype(jnp.int32),
        "kappa_table": jnp.clip(jnp.exp(jax.random.uniform(keys[3], (SPECIES,), jnp.float32, math.log(0.1), math.log(1.0))), 0.1, 1.0),
        "dealias_bound": plant(jax.random.randint(keys[4], (SCALARS,), N // 4, N // 3 + 1), jax.random.fold_in(keys[4], 1), N // 4, (N // 3 + 1) - 1).astype(jnp.int32),
    }


cfl_number = 0.2

def twiddle(size_in, size_out, length):
    row_index = jnp.arange(size_in, dtype=jnp.int32)[:, None]
    col_index = jnp.arange(size_out, dtype=jnp.int32)[None, :]
    angles = (row_index * col_index % length).astype(jnp.float32) * (2.0 * math.pi / length)
    norming = 1.0 / math.sqrt(length)
    return (jnp.cos(angles) * norming, jnp.sin(angles) * norming)

def build_tables(length):
    half_len = length // 2
    full_cos, full_sin = twiddle(length, length, length)
    inv_cos, inv_sin = twiddle(half_len, length, length)
    weight = jnp.where(jnp.arange(half_len, dtype=jnp.int32) == 0, 1.0, 2.0).astype(jnp.float32)[:, None]
    fwd_cos, fwd_sin = twiddle(length, half_len, length)
    listed = (full_cos, full_sin, inv_cos * weight, inv_sin * weight, fwd_cos, fwd_sin)
    return tuple((matrix.astype(jnp.bfloat16) for matrix in listed))

def product(formula, operand, matrix):
    return jnp.einsum(formula, operand.astype(jnp.float32), matrix.astype(jnp.float32), precision=lax.Precision.HIGHEST)

def complex_section(real_part, imag_part, cos_matrix, sin_matrix, formula, inverse):
    real_cos = product(formula, real_part, cos_matrix)
    real_sin = product(formula, real_part, sin_matrix)
    imag_cos = product(formula, imag_part, cos_matrix)
    imag_sin = product(formula, imag_part, sin_matrix)
    if inverse:
        return (real_cos - imag_sin, real_sin + imag_cos)
    return (real_cos + imag_sin, imag_cos - real_sin)

def reference(scalar_state, velocity, species, kappa_table, dealias_bound):
    scalar_count = scalar_state.shape[0]
    table_count = kappa_table.shape[0]
    length = scalar_state.shape[2]
    half_len = length // 2
    full_cos, full_sin, inv_cos, inv_sin, fwd_cos, fwd_sin = build_tables(length)
    index_full = jnp.arange(length, dtype=jnp.int32)
    signed = jnp.where(index_full < half_len, index_full, index_full - length).astype(jnp.float32)
    ky_wave = signed[:, None, None]
    kz_wave = signed[None, :, None]
    kx_wave = jnp.arange(half_len, dtype=jnp.int32).astype(jnp.float32)[None, None, :]
    ksquare = kx_wave * kx_wave + ky_wave * ky_wave + kz_wave * kz_wave
    weight = jnp.where(kx_wave == 0.0, 1.0, 2.0).astype(jnp.float32)
    cell_count = float(length) ** 3
    step_size = cfl_number * 2.0 * math.pi / length

    def z_inverse(real_part, imag_part):
        z_section = complex_section(real_part, imag_part, full_cos, full_sin, 'ykx,kz->yzx', True)
        return (z_section[0].astype(jnp.bfloat16), z_section[1].astype(jnp.bfloat16))

    def rest_inverse(real_part, imag_part):
        y_section = complex_section(real_part, imag_part, full_cos, full_sin, 'yzx,yw->zwx', True)
        y_real = y_section[0].astype(jnp.bfloat16)
        y_imag = y_section[1].astype(jnp.bfloat16)
        return product('zwk,kx->zwx', y_real, inv_cos) - product('zwk,kx->zwx', y_imag, inv_sin)

    def gradient_set(real_part, imag_part):
        whole_real, whole_imag = z_inverse(real_part.astype(jnp.bfloat16), imag_part.astype(jnp.bfloat16))
        deriv_real, deriv_imag = z_inverse((-kz_wave * imag_part).astype(jnp.bfloat16), (kz_wave * real_part).astype(jnp.bfloat16))
        results = []
        for wavenumber in (kx_wave, ky_wave):
            grad_real = (-wavenumber * whole_imag.astype(jnp.float32)).astype(jnp.bfloat16)
            grad_imag = (wavenumber * whole_real.astype(jnp.float32)).astype(jnp.bfloat16)
            results.append(rest_inverse(grad_real, grad_imag))
        results.append(rest_inverse(deriv_real, deriv_imag))
        return results

    def advect(gradients):
        total = velocity[0].astype(jnp.float32) * gradients[0]
        total = total + velocity[1].astype(jnp.float32) * gradients[1]
        total = total + velocity[2].astype(jnp.float32) * gradients[2]
        return total.astype(jnp.bfloat16)

    def forward_field(physical):
        real_x = product('zyx,xk->zyk', physical, fwd_cos).astype(jnp.bfloat16)
        imag_x = (-product('zyx,xk->zyk', physical, fwd_sin)).astype(jnp.bfloat16)
        y_section = complex_section(real_x, imag_x, full_cos, full_sin, 'zyk,yw->wzk', False)
        y_real = y_section[0].astype(jnp.bfloat16)
        y_imag = y_section[1].astype(jnp.bfloat16)
        return complex_section(y_real, y_imag, full_cos, full_sin, 'wzk,zv->wvk', False)
    updated_list = []
    kappa_list = []
    for scalar in range(scalar_count):
        start_real = scalar_state[scalar, 0]
        start_imag = scalar_state[scalar, 1]
        energy = start_real * start_real + start_imag * start_imag
        variance = jnp.sum(weight * energy) / cell_count
        mean_grad = jnp.sum(weight * ksquare * energy) / cell_count
        gradients = gradient_set(start_real, start_imag)
        peak_value = jnp.max(jnp.sqrt(gradients[0] * gradients[0] + gradients[1] * gradients[1] + gradients[2] * gradients[2]))
        base_kappa = jnp.sum(jnp.where(species[scalar] == jnp.arange(table_count, dtype=jnp.int32), kappa_table, 0.0))
        kappa_value = base_kappa * peak_value * jnp.sqrt(variance) / (mean_grad + 1e-06)
        factor = jnp.exp(-kappa_value * ksquare * step_size)
        bound = dealias_bound[scalar].astype(jnp.float32)
        dealias_mask = (ksquare <= bound * bound).astype(jnp.float32)
        first_real, first_imag = forward_field(advect(gradients))
        first_real = -dealias_mask * first_real
        first_imag = -dealias_mask * first_imag
        mid_real = factor * (start_real + step_size * first_real)
        mid_imag = factor * (start_imag + step_size * first_imag)
        second_real, second_imag = forward_field(advect(gradient_set(mid_real, mid_imag)))
        second_real = -dealias_mask * second_real
        second_imag = -dealias_mask * second_imag
        new_real = factor * start_real + 0.5 * step_size * (factor * first_real + second_real)
        new_imag = factor * start_imag + 0.5 * step_size * (factor * first_imag + second_imag)
        updated_list.append(jnp.stack([new_real, new_imag]))
        kappa_list.append(kappa_value)
    return (jnp.stack(updated_list), jnp.stack(kappa_list))
```

```python
import functools
import math

import jax
import jax.numpy as jnp
import numpy as np
from jax import lax
from jax.experimental import pallas as pl
from jax.experimental.pallas import tpu as pltpu
from jax.sharding import PartitionSpec as P

MESH = pl.DeviceIdType.MESH
cfl_number = 0.2
LARGEST_BOUND = 85
F32, BF16 = jnp.float32, jnp.bfloat16


def base_tables(length):
    index = np.arange(length)
    angles = (index[:, None] * index[None, :] % length).astype(np.float32) * np.float32(2.0 * math.pi / length)
    norming = np.float32(1.0 / math.sqrt(length))
    cos = (np.cos(angles).astype(np.float32) * norming).astype(np.float32)
    sin = (np.sin(angles).astype(np.float32) * norming).astype(np.float32)
    return cos, sin


def kept_slabs(length, parts):
    rows = length // parts
    signed = np.where(np.arange(length) < length // 2, np.arange(length), np.arange(length) - length)
    return [d for d in range(parts) if np.min(np.abs(signed[d * rows : (d + 1) * rows])) <= LARGEST_BOUND]


def build_tables(length, parts):
    cos, sin = base_tables(length)
    half, rows = length // 2, length // parts
    weight = np.where(np.arange(half) == 0, 1.0, 2.0).astype(np.float32)[:, None]
    real = np.stack([cos, -sin], axis=1)
    imag = np.stack([sin, cos], axis=1)
    inverse = np.stack([real, imag]).transpose(0, 3, 2, 1)
    turned = np.stack([np.stack([-sin, -cos], 1), np.stack([cos, -sin], 1)]).transpose(0, 3, 2, 1)
    forward = np.stack([np.stack([cos, sin], 1), np.stack([-sin, cos], 1)]).transpose(0, 3, 2, 1)
    size = 2 * length

    def slab_columns(table):
        return table.reshape(size, 2, parts, rows).transpose(0, 2, 1, 3).reshape(size, size)

    def slab_rows(table):
        return table.transpose(1, 0, 2, 3).reshape(size, size)

    kept = kept_slabs(length, parts)
    z_inv = slab_rows(inverse)
    y_inv = slab_columns(inverse)
    y_inv_turned = slab_columns(turned)
    y_fwd = slab_rows(forward).reshape(parts, 2 * rows, size)[kept].reshape(-1, size)
    z_fwd = slab_columns(forward)
    x_inv = np.concatenate([cos[:half] * weight, -(sin[:half] * weight)], axis=0)
    x_fwd = np.concatenate([cos[:, :half], -sin[:, :half]], axis=1)
    listed = (z_inv, y_inv, y_inv_turned, y_fwd, z_fwd, x_inv, x_fwd)
    return tuple(jnp.asarray(t.astype(np.float32)).astype(BF16) for t in listed)


def dot(a, b):
    return jnp.dot(a, b, preferred_element_type=F32)


def signed_of(index, length):
    return jnp.where(index < length // 2, index, index - length).astype(F32)


def kernel(
    parts, groups, near,
    state, velocity, species, table, bound,
    z_inv, y_inv, y_inv_turned, y_fwd, z_fwd, x_inv, x_fwd,
    out, kappa_out,
    spec, work, sent, came, speeds, grads, lines, flat, back_sent, back_came, stats,
    send_sem, came_sem, back_send_sem, back_sem, stat_send_sem, stat_sem, vel_sem, vel_send, vel_recv,
):
    rows, length, half = state.shape[1], state.shape[2], state.shape[3]
    kept = kept_slabs(length, parts)
    low = sum(1 for d in kept if d < parts // 2)
    gap = parts - len(kept)
    planes = length // parts
    pairs = planes // 2
    step_size = cfl_number * 2.0 * math.pi / length
    cell_count = float(length) ** 3
    me = lax.axis_index("fft")
    mine = lax.axis_index("scal")
    far = lax.rem(mine + groups // 2, groups)
    upper = (mine // near) * near
    up = upper + lax.rem(mine + 1, near)
    down = upper + lax.rem(mine + near - 1, near)
    far_up, far_down = lax.rem(up + groups // 2, groups), lax.rem(down + groups // 2, groups)
    across = upper + lax.rem(mine + 2, near)
    far_across = lax.rem(across + groups // 2, groups)

    barrier = pltpu.get_barrier_semaphore()

    @pl.loop(1, parts)
    def _(k):
        pl.semaphore_signal(barrier, inc=1, device_id={"fft": lax.rem(me + k, parts)}, device_id_type=MESH)

    for peer in (far, up, down):
        pl.semaphore_signal(barrier, inc=1, device_id={"scal": peer}, device_id_type=MESH)

    own_speeds = pltpu.make_async_copy(velocity, speeds.at[mine], vel_sem)
    own_speeds.start()

    kz = signed_of(lax.broadcasted_iota(jnp.int32, (length, 1), 0), length)
    kx_index = lax.broadcasted_iota(jnp.int32, (1, half), 1)
    kx = kx_index.astype(F32)
    weight = jnp.where(kx_index == 0, 1.0, 2.0).astype(F32)

    def square(row):
        ky = signed_of(me * rows + row, length)
        return kx * kx + ky * ky + kz * kz

    def put_spectrum(row, real, imag):
        spec[row, :length, :half] = real.astype(BF16)
        spec[row, length:, :half] = imag.astype(BF16)
        spec[row, :length, half:] = (-kz * imag).astype(BF16)
        spec[row, length:, half:] = (kz * real).astype(BF16)

    def fold(x):
        return jnp.sum(x.reshape(length // 8, 8, half), axis=0)

    def first_row(row, total):
        real, imag = state[0, row], state[1, row]
        put_spectrum(row, real, imag)
        energy = weight * (real * real + imag * imag)
        return total[0] + fold(energy), total[1] + fold(square(row) * energy)

    zero = jnp.zeros((8, half), F32)
    variance_part, grad_part = lax.fori_loop(0, rows, first_row, (zero, zero))

    batch = 8
    batch_rows = batch * 2 * planes

    def came_copy(turn, chunk, peer):
        return pltpu.make_async_remote_copy(
            src_ref=sent.at[peer, pl.ds(2 * chunk, 2)],
            dst_ref=came.at[pl.ds(2 * chunk, 2), me],
            send_sem=send_sem.at[turn],
            recv_sem=came_sem.at[turn * pairs + chunk],
            device_id={"fft": peer},
            device_id_type=MESH,
        )

    def send_planes(turn):
        def one_batch(k, _):
            which = lax.rem(me // batch + k, parts // batch)
            at = pl.multiple_of(which * batch_rows, batch_rows)

            @pl.loop(0, rows)
            def _(row):
                work[row] = dot(z_inv[pl.ds(at, batch_rows), :], spec[row])

            @pl.loop(0, batch)
            def _(j):
                peer = which * batch + j
                start = pl.multiple_of(j * 2 * planes, 2 * planes)
                block = work[:, pl.ds(start, 2 * planes), :]
                turned = jnp.swapaxes(block, 0, 1).reshape(planes, 2 * rows, 2 * half).astype(BF16)
                sent[peer] = turned

                @pl.when(peer == me)
                def _():
                    came[:, pl.ds(me, 1)] = turned[:, None]

            if turn == 0:
                @pl.when(k == 0)
                def _():
                    pl.semaphore_wait(barrier, parts - 1 + 3)

            @pl.loop(0, batch)
            def _(j):
                peer = which * batch + j

                @pl.when(peer != me)
                def _():
                    came_copy(turn, 0, peer).start()

            return 0

        lax.fori_loop(0, parts // batch, one_batch, 0)

        @pl.loop(1, pairs)
        def _(chunk):
            @pl.loop(1, parts)
            def _(k):
                came_copy(turn, chunk, lax.rem(me + k, parts)).start()

    def wait_planes(turn, chunk):
        piece = sent.at[pl.ds(0, parts - 1), pl.ds(0, 2)]
        pltpu.make_async_remote_copy(
            src_ref=piece, dst_ref=piece, send_sem=send_sem.at[turn],
            recv_sem=came_sem.at[turn * pairs + chunk], device_id={"fft": me}, device_id_type=MESH,
        ).wait_recv()

    def wait_sent(turn):
        piece = sent.at[pl.ds(0, parts - 1)]
        pltpu.make_async_remote_copy(
            src_ref=piece, dst_ref=piece, send_sem=send_sem.at[turn],
            recv_sem=came_sem.at[turn * pairs], device_id={"fft": me}, device_id_type=MESH,
        ).wait_send()

    ky_row = lax.broadcasted_iota(jnp.int32, (2 * length, 1), 0)
    ky_row = signed_of((ky_row // (2 * rows)) * rows + lax.rem(ky_row, rows), length).astype(BF16)
    kx_low = kx.astype(BF16)

    def to_grid(field, plane, real, imag):
        halves = jnp.concatenate([real, imag], axis=1).astype(BF16)
        grads[field, plane] = dot(halves, x_inv[...])

    def gradient_pair(chunk):
        last = []
        for side in (0, 1):
            plane = 2 * chunk + side
            both = came[plane].reshape(2 * length, 2 * half)
            whole, deriv = both[:, :half], both[:, half:]
            last.append(deriv)
            scaled = jnp.concatenate([whole * kx_low, whole * ky_row], axis=1)
            done = dot(y_inv_turned[...], scaled)
            to_grid(0, plane, done[:length, :half], done[length:, :half])
            to_grid(1, plane, done[:length, half:], done[length:, half:])
        done = dot(y_inv[...], jnp.concatenate(last, axis=1))
        to_grid(2, 2 * chunk, done[:length, :half], done[length:, :half])
        to_grid(2, 2 * chunk + 1, done[:length, half:], done[length:, half:])

    def peak_of(plane, peak):
        gx, gy, gz = grads[0, plane], grads[1, plane], grads[2, plane]
        size = gx * gx + gy * gy + gz * gz
        return jnp.maximum(peak, jnp.max(size.reshape(-1, 8, length), axis=0))

    def forward_pair(chunk):
        for side in (0, 1):
            plane = 2 * chunk + side
            total = speeds[:, 0, plane].reshape(length, length).astype(F32) * grads[0, plane]
            total = total + speeds[:, 1, plane].reshape(length, length).astype(F32) * grads[1, plane]
            total = total + speeds[:, 2, plane].reshape(length, length).astype(F32) * grads[2, plane]
            part = dot(total.astype(BF16), x_fwd[...]).astype(BF16)
            lines[:length, side * half : (side + 1) * half] = part[:, :half]
            lines[length:, side * half : (side + 1) * half] = part[:, half:]
        done = dot(y_fwd[...], lines[...])
        flat[2 * chunk] = done[:, :half]
        flat[2 * chunk + 1] = done[:, half:]

    def back_copy(turn, slot, peer):
        return pltpu.make_async_remote_copy(
            src_ref=back_sent.at[slot], dst_ref=back_came.at[me],
            send_sem=back_send_sem.at[turn], recv_sem=back_sem.at[turn],
            device_id={"fft": peer}, device_id_type=MESH,
        )

    keeps = jnp.logical_or(me < low, me >= low + gap)

    def send_rows(turn):
        @pl.loop(0, len(kept))
        def _(slot):
            peer = jnp.where(slot < low, slot, slot + gap)
            start = pl.multiple_of(slot * 2 * rows, 2 * rows)
            block = flat[:, pl.ds(start, 2 * rows), :]
            turned = jnp.swapaxes(block, 0, 1).reshape(rows, 2 * planes, half).astype(BF16)
            back_sent[slot] = turned

            @pl.when(peer == me)
            def _():
                back_came[pl.ds(me, 1)] = turned[None]

            @pl.when(peer != me)
            def _():
                back_copy(turn, slot, peer).start()

    def wait_rows_sent(turn):
        @pl.when(keeps)
        def _():
            piece = back_sent.at[pl.ds(0, len(kept) - 1)]
            pltpu.make_async_remote_copy(
                src_ref=piece, dst_ref=piece, send_sem=back_send_sem.at[turn],
                recv_sem=back_sem.at[turn], device_id={"fft": me}, device_id_type=MESH,
            ).wait_send()

        @pl.when(jnp.logical_not(keeps))
        def _():
            piece = back_sent.at[pl.ds(0, len(kept))]
            pltpu.make_async_remote_copy(
                src_ref=piece, dst_ref=piece, send_sem=back_send_sem.at[turn],
                recv_sem=back_sem.at[turn], device_id={"fft": me}, device_id_type=MESH,
            ).wait_send()

    def wait_rows(turn):
        @pl.when(keeps)
        def _():
            piece = back_came.at[pl.ds(0, parts - 1)]
            pltpu.make_async_remote_copy(
                src_ref=piece, dst_ref=piece, send_sem=back_send_sem.at[turn],
                recv_sem=back_sem.at[turn], device_id={"fft": me}, device_id_type=MESH,
            ).wait_recv()

    def tendency_pair(pair):
        held = [back_came[:, 2 * pair + side].reshape(2 * length, half) for side in (0, 1)]
        return dot(z_fwd[...], jnp.concatenate(held, axis=1))

    def speeds_copy(k, block, peer, at=None):
        ref = speeds.at[block] if at is None else speeds.at[block, :, pl.ds(at, planes // 2)]
        return pltpu.make_async_remote_copy(
            src_ref=ref, dst_ref=ref, send_sem=vel_send.at[k], recv_sem=vel_recv.at[k],
            device_id={"scal": peer}, device_id_type=MESH,
        )

    @pl.when(jnp.logical_not(keeps))
    def _():
        back_came[...] = jnp.zeros_like(back_came)

    own_speeds.wait()
    send_planes(0)
    first = speeds_copy(0, mine, far)
    first.start()
    first.wait_send()
    speeds_copy(0, far, far).wait_recv()
    for k, peer in ((1, up), (3, down)):
        speeds_copy(k, mine, peer).start()
        speeds_copy(k + 1, far, peer).start()

    def half_one(chunk, peak):
        wait_planes(0, chunk)
        gradient_pair(chunk)
        return peak_of(2 * chunk + 1, peak_of(2 * chunk, peak))

    peak = jnp.zeros((8, length), F32)
    peak = lax.fori_loop(0, pairs // 2, half_one, peak)
    cut = planes // 2
    speeds_copy(1, down, up).wait_recv()
    speeds_copy(2, far_down, up).wait_recv()
    speeds_copy(5, down, up, 0).start()
    speeds_copy(6, far_down, up, 0).start()
    speeds_copy(3, up, down).wait_recv()
    speeds_copy(4, far_up, down).wait_recv()
    speeds_copy(7, up, down, cut).start()
    speeds_copy(8, far_up, down, cut).start()
    peak = lax.fori_loop(pairs // 2, pairs, half_one, peak)
    for k, peer in ((1, up), (3, down)):
        speeds_copy(k, mine, peer).wait_send()
        speeds_copy(k + 1, far, peer).wait_send()
    speeds_copy(5, across, up, 0).wait()
    speeds_copy(6, far_across, up, 0).wait()
    speeds_copy(7, across, down, cut).wait()
    speeds_copy(8, far_across, down, cut).wait()

    peak = jnp.maximum(peak[:, :half], peak[:, half:])
    stats[me] = jnp.concatenate(
        [
            jnp.sum(variance_part, axis=0, keepdims=True),
            jnp.sum(grad_part, axis=0, keepdims=True),
            jnp.max(peak, axis=0, keepdims=True),
            jnp.zeros((5, half), F32),
        ],
        axis=0,
    )

    @pl.loop(0, pairs)
    def _(chunk):
        forward_pair(chunk)

    @pl.loop(1, parts)
    def _(k):
        pltpu.make_async_remote_copy(
            src_ref=stats.at[me], dst_ref=stats.at[me], send_sem=stat_send_sem, recv_sem=stat_sem,
            device_id={"fft": lax.rem(me + k, parts)}, device_id_type=MESH,
        ).start()

    send_rows(0)
    wait_sent(0)
    everyone = stats.at[pl.ds(0, parts - 1)]
    stat_wait = pltpu.make_async_remote_copy(
        src_ref=everyone, dst_ref=everyone, send_sem=stat_send_sem, recv_sem=stat_sem,
        device_id={"fft": me}, device_id_type=MESH,
    )
    stat_wait.wait_send()
    stat_wait.wait_recv()
    collected = stats[...]
    variance = jnp.sum(jnp.sum(collected[:, 0], axis=0, keepdims=True), axis=1, keepdims=True) / cell_count
    mean_grad = jnp.sum(jnp.sum(collected[:, 1], axis=0, keepdims=True), axis=1, keepdims=True) / cell_count
    largest = jnp.max(jnp.max(collected[:, 2], axis=0, keepdims=True), axis=1, keepdims=True)
    count = table.shape[1]
    match = lax.broadcasted_iota(jnp.int32, (1, count), 1) == species[0]
    base = jnp.sum(jnp.where(match, table[...], 0.0), axis=1, keepdims=True)
    kappa = base * jnp.sqrt(largest) * jnp.sqrt(variance) / (mean_grad + 1e-06)
    kappa_out[...] = jnp.broadcast_to(kappa, kappa_out.shape)
    limit = bound[0].astype(F32)
    limit = limit * limit

    wait_rows(0)

    @pl.loop(0, rows // 2)
    def _(pair):
        done = tendency_pair(pair)
        for side in (0, 1):
            row = 2 * pair + side
            here = slice(side * half, (side + 1) * half)
            ksquare = square(row)
            keep = ksquare <= limit
            factor = jnp.exp(-kappa * ksquare * step_size)
            moved = []
            for part in (0, 1):
                start = state[part, row]
                rate = jnp.where(keep, -done[part * length : (part + 1) * length, here], 0.0)
                moved.append(factor * (start + step_size * rate))
                out[part, row] = factor * start + 0.5 * step_size * (factor * rate)
            put_spectrum(row, *moved)

    send_planes(1)

    @pl.loop(0, pairs)
    def _(chunk):
        wait_planes(1, chunk)
        gradient_pair(chunk)
        forward_pair(chunk)

    wait_rows_sent(0)
    send_rows(1)
    wait_sent(1)
    wait_rows(1)

    @pl.loop(0, rows // 2)
    def _(pair):
        done = tendency_pair(pair)
        for side in (0, 1):
            row = 2 * pair + side
            here = slice(side * half, (side + 1) * half)
            keep = square(row) <= limit
            for part in (0, 1):
                rate = jnp.where(keep, -done[part * length : (part + 1) * length, here], 0.0)
                out[part, row] = out[part, row] + 0.5 * step_size * rate

    wait_rows_sent(1)


def body(parts, groups, scalar_state, velocity, species, kappa_table, dealias_bound):
    _, _, rows, length, half = scalar_state.shape
    planes = length // parts
    kept = kept_slabs(length, parts)
    tables = build_tables(length, parts)
    near = groups // 2
    chunk_rows = velocity.shape[2]
    vmem = pl.BlockSpec(memory_space=pltpu.VMEM)
    smem = pl.BlockSpec(memory_space=pltpu.SMEM)
    hbm = pl.BlockSpec(memory_space=pl.ANY)
    DMA = pltpu.SemaphoreType.DMA
    new_state, kappa = pl.pallas_call(
        functools.partial(kernel, parts, groups, near),
        out_shape=(
            jax.ShapeDtypeStruct((2, rows, length, half), F32),
            jax.ShapeDtypeStruct((8, half), F32),
        ),
        in_specs=[vmem, hbm, smem, vmem, smem] + [vmem] * len(tables),
        out_specs=(vmem, vmem),
        scratch_shapes=[
            pltpu.VMEM((rows, 2 * length, 2 * half), BF16),
            pltpu.VMEM((rows, 16 * planes, 2 * half), F32),
            pltpu.VMEM((parts, planes, 2 * rows, 2 * half), BF16),
            pltpu.VMEM((planes, parts, 2 * rows, 2 * half), BF16),
            pltpu.VMEM((groups, 3, planes, chunk_rows, length), BF16),
            pltpu.VMEM((3, planes, length, length), F32),
            pltpu.VMEM((2 * length, 2 * half), BF16),
            pltpu.VMEM((planes, len(kept) * 2 * rows, half), F32),
            pltpu.VMEM((len(kept), rows, 2 * planes, half), BF16),
            pltpu.VMEM((parts, rows, 2 * planes, half), BF16),
            pltpu.VMEM((parts, 8, half), F32),
            DMA((2,)),
            DMA((planes,)),
            DMA((2,)),
            DMA((2,)),
            DMA,
            DMA,
            DMA,
            DMA((9,)),
            DMA((9,)),
        ],
        compiler_params=pltpu.CompilerParams(
            collective_id=0, has_side_effects=True, vmem_limit_bytes=60 * 1024 * 1024
        ),
    )(scalar_state[0], velocity, species, kappa_table[None, :], dealias_bound, *tables)
    return new_state[None], kappa[0, :1]


def solution(mesh):
    parts, groups = mesh.shape["fft"], mesh.shape["scal"]
    placed = (
        P("scal", None, "fft", None, None),
        P(None, "fft", "scal", None),
        P("scal"),
        P(),
        P("scal"),
    )
    return jax.shard_map(
        functools.partial(body, parts, groups),
        mesh=mesh,
        in_specs=placed,
        out_specs=(P("scal", None, "fft", None, None), P("scal")),
        check_vma=False,
    )
```

```python
import functools
import math

import jax
import jax.numpy as jnp
import numpy as np
from jax import lax
from jax.experimental import pallas as pl
from jax.experimental.pallas import tpu as pltpu
from jax.sharding import PartitionSpec as P

MESH = pl.DeviceIdType.MESH
cfl_number = 0.2
LARGEST_BOUND = 85
F32, BF16 = jnp.float32, jnp.bfloat16


def base_tables(length):
    index = np.arange(length)
    angles = (index[:, None] * index[None, :] % length).astype(np.float32) * np.float32(2.0 * math.pi / length)
    norming = np.float32(1.0 / math.sqrt(length))
    cos = (np.cos(angles).astype(np.float32) * norming).astype(np.float32)
    sin = (np.sin(angles).astype(np.float32) * norming).astype(np.float32)
    return cos, sin


def kept_slabs(length, parts):
    rows = length // parts
    signed = np.where(np.arange(length) < length // 2, np.arange(length), np.arange(length) - length)
    return [d for d in range(parts) if np.min(np.abs(signed[d * rows : (d + 1) * rows])) <= LARGEST_BOUND]


def narrow_slots(length, parts, half):
    rows = length // parts
    thin = []
    for slot, d in enumerate(kept_slabs(length, parts)):
        ky = np.arange(d * rows, (d + 1) * rows)
        least = np.min(np.abs(np.where(ky < length // 2, ky, ky - length)))
        if LARGEST_BOUND**2 - least**2 < (half // 2) ** 2:
            thin.append(slot)
    assert thin == list(range(thin[0], thin[-1] + 1))
    return thin[0], thin[-1] + 1


def build_tables(length, parts):
    cos, sin = base_tables(length)
    half, rows = length // 2, length // parts
    weight = np.where(np.arange(half) == 0, 1.0, 2.0).astype(np.float32)[:, None]
    real = np.stack([cos, -sin], axis=1)
    imag = np.stack([sin, cos], axis=1)
    inverse = np.stack([real, imag]).transpose(0, 3, 2, 1)
    turned = np.stack([np.stack([-sin, -cos], 1), np.stack([cos, -sin], 1)]).transpose(0, 3, 2, 1)
    forward = np.stack([np.stack([cos, sin], 1), np.stack([-sin, cos], 1)]).transpose(0, 3, 2, 1)
    size = 2 * length

    def slab_columns(table):
        return table.reshape(size, 2, parts, rows).transpose(0, 2, 1, 3).reshape(size, size)

    def slab_rows(table):
        return table.transpose(1, 0, 2, 3).reshape(size, size)

    kept = kept_slabs(length, parts)
    z_inv = slab_rows(inverse)
    y_inv = slab_columns(inverse)
    y_inv_turned = slab_columns(turned)
    y_fwd = slab_rows(forward).reshape(parts, 2 * rows, size)[kept].reshape(-1, size)
    z_fwd = slab_columns(forward)
    x_inv = np.concatenate([cos[:half] * weight, -(sin[:half] * weight)], axis=0)
    x_fwd = np.concatenate([cos[:, :half], -sin[:, :half]], axis=1)
    listed = (z_inv, y_inv, y_inv_turned, y_fwd, z_fwd, x_inv, x_fwd)
    return tuple(jnp.asarray(t.astype(np.float32)).astype(BF16) for t in listed)


def dot(a, b):
    return jnp.dot(a, b, preferred_element_type=F32)


def signed_of(index, length):
    return jnp.where(index < length // 2, index, index - length).astype(F32)


def kernel(
    parts, groups, near,
    state, velocity, species, table, bound,
    z_inv, y_inv, y_inv_turned, y_fwd, z_fwd, x_inv, x_fwd,
    out, kappa_out,
    spec, work, sent, came, speeds, grads, lines, flat, back_sent, back_came, stats,
    send_sem, came_sem, back_send_sem, back_sem, stat_send_sem, stat_sem, vel_sem, vel_send, vel_recv,
):
    rows, length, half = state.shape[1], state.shape[2], state.shape[3]
    kept = kept_slabs(length, parts)
    low = sum(1 for d in kept if d < parts // 2)
    gap = parts - len(kept)
    planes = length // parts
    pairs = planes // 2
    step_size = cfl_number * 2.0 * math.pi / length
    cell_count = float(length) ** 3
    me = lax.axis_index("fft")
    mine = lax.axis_index("scal")
    far = lax.rem(mine + groups // 2, groups)
    upper = (mine // near) * near
    up = upper + lax.rem(mine + 1, near)
    down = upper + lax.rem(mine + near - 1, near)
    far_up, far_down = lax.rem(up + groups // 2, groups), lax.rem(down + groups // 2, groups)
    across = upper + lax.rem(mine + 2, near)
    far_across = lax.rem(across + groups // 2, groups)

    barrier = pltpu.get_barrier_semaphore()

    @pl.loop(1, parts)
    def _(k):
        pl.semaphore_signal(barrier, inc=1, device_id={"fft": lax.rem(me + k, parts)}, device_id_type=MESH)

    for peer in (far, up, down):
        pl.semaphore_signal(barrier, inc=1, device_id={"scal": peer}, device_id_type=MESH)

    own_speeds = pltpu.make_async_copy(velocity, speeds.at[mine], vel_sem)
    own_speeds.start()

    kz = signed_of(lax.broadcasted_iota(jnp.int32, (length, 1), 0), length)
    kx_index = lax.broadcasted_iota(jnp.int32, (1, half), 1)
    kx = kx_index.astype(F32)
    weight = jnp.where(kx_index == 0, 1.0, 2.0).astype(F32)

    def square(row):
        ky = signed_of(me * rows + row, length)
        return kx * kx + ky * ky + kz * kz

    def put_spectrum(row, real, imag):
        spec[row, :length, :half] = real.astype(BF16)
        spec[row, length:, :half] = imag.astype(BF16)
        spec[row, :length, half:] = (-kz * imag).astype(BF16)
        spec[row, length:, half:] = (kz * real).astype(BF16)

    def fold(x):
        return jnp.sum(x.reshape(length // 8, 8, half), axis=0)

    def first_row(row, total):
        real, imag = state[0, row], state[1, row]
        put_spectrum(row, real, imag)
        energy = weight * (real * real + imag * imag)
        return total[0] + fold(energy), total[1] + fold(square(row) * energy)

    zero = jnp.zeros((8, half), F32)
    variance_part, grad_part = lax.fori_loop(0, rows, first_row, (zero, zero))

    batch = 8
    batch_rows = batch * 2 * planes

    def came_copy(turn, chunk, peer):
        return pltpu.make_async_remote_copy(
            src_ref=sent.at[peer, pl.ds(2 * chunk, 2)],
            dst_ref=came.at[pl.ds(2 * chunk, 2), me],
            send_sem=send_sem.at[turn],
            recv_sem=came_sem.at[turn * pairs + chunk],
            device_id={"fft": peer},
            device_id_type=MESH,
        )

    def send_planes(turn):
        def one_batch(k, _):
            which = lax.rem(me // batch + k, parts // batch)
            at = pl.multiple_of(which * batch_rows, batch_rows)

            @pl.loop(0, rows)
            def _(row):
                work[row] = dot(z_inv[pl.ds(at, batch_rows), :], spec[row])

            @pl.loop(0, batch)
            def _(j):
                peer = which * batch + j
                start = pl.multiple_of(j * 2 * planes, 2 * planes)
                block = work[:, pl.ds(start, 2 * planes), :]
                turned = jnp.swapaxes(block, 0, 1).reshape(planes, 2 * rows, 2 * half).astype(BF16)
                sent[peer] = turned

                @pl.when(peer == me)
                def _():
                    came[:, pl.ds(me, 1)] = turned[:, None]

            if turn == 0:
                @pl.when(k == 0)
                def _():
                    pl.semaphore_wait(barrier, parts - 1 + 3)
                    speeds_copy(0, mine, far).start()

            @pl.loop(0, batch)
            def _(j):
                peer = which * batch + j

                @pl.when(peer != me)
                def _():
                    came_copy(turn, 0, peer).start()

            return 0

        lax.fori_loop(0, parts // batch, one_batch, 0)

        @pl.loop(1, pairs)
        def _(chunk):
            @pl.loop(1, parts)
            def _(k):
                came_copy(turn, chunk, lax.rem(me + k, parts)).start()

    def wait_planes(turn, chunk):
        piece = sent.at[pl.ds(0, parts - 1), pl.ds(0, 2)]
        pltpu.make_async_remote_copy(
            src_ref=piece, dst_ref=piece, send_sem=send_sem.at[turn],
            recv_sem=came_sem.at[turn * pairs + chunk], device_id={"fft": me}, device_id_type=MESH,
        ).wait_recv()

    def wait_sent(turn):
        piece = sent.at[pl.ds(0, parts - 1)]
        pltpu.make_async_remote_copy(
            src_ref=piece, dst_ref=piece, send_sem=send_sem.at[turn],
            recv_sem=came_sem.at[turn * pairs], device_id={"fft": me}, device_id_type=MESH,
        ).wait_send()

    ky_row = lax.broadcasted_iota(jnp.int32, (2 * length, 1), 0)
    ky_row = signed_of((ky_row // (2 * rows)) * rows + lax.rem(ky_row, rows), length).astype(BF16)
    kx_low = kx.astype(BF16)

    def to_grid(field, plane, real, imag):
        halves = jnp.concatenate([real, imag], axis=1).astype(BF16)
        grads[field, plane] = dot(halves, x_inv[...])

    def gradient_pair(chunk):
        last = []
        for side in (0, 1):
            plane = 2 * chunk + side
            both = came[plane].reshape(2 * length, 2 * half)
            whole, deriv = both[:, :half], both[:, half:]
            last.append(deriv)
            scaled = jnp.concatenate([whole * kx_low, whole * ky_row], axis=1)
            done = dot(y_inv_turned[...], scaled)
            to_grid(0, plane, done[:length, :half], done[length:, :half])
            to_grid(1, plane, done[:length, half:], done[length:, half:])
        done = dot(y_inv[...], jnp.concatenate(last, axis=1))
        to_grid(2, 2 * chunk, done[:length, :half], done[length:, :half])
        to_grid(2, 2 * chunk + 1, done[:length, half:], done[length:, half:])

    def peak_of(plane, peak):
        gx, gy, gz = grads[0, plane], grads[1, plane], grads[2, plane]
        size = gx * gx + gy * gy + gz * gz
        return jnp.maximum(peak, jnp.max(size.reshape(-1, 8, length), axis=0))

    def forward_pair(chunk):
        for side in (0, 1):
            plane = 2 * chunk + side
            total = speeds[:, 0, plane].reshape(length, length).astype(F32) * grads[0, plane]
            total = total + speeds[:, 1, plane].reshape(length, length).astype(F32) * grads[1, plane]
            total = total + speeds[:, 2, plane].reshape(length, length).astype(F32) * grads[2, plane]
            part = dot(total.astype(BF16), x_fwd[...]).astype(BF16)
            lines[:length, side * half : (side + 1) * half] = part[:, :half]
            lines[length:, side * half : (side + 1) * half] = part[:, half:]
        done = dot(y_fwd[...], lines[...])
        flat[2 * chunk] = done[:, :half]
        flat[2 * chunk + 1] = done[:, half:]

    quads = rows // 4
    keeps = jnp.logical_or(me < low, me >= low + gap)
    my_slot = jnp.where(me < low, me, me - gap)
    thin_low, thin_high = narrow_slots(length, parts, half)
    my_thin = jnp.logical_and(keeps, jnp.logical_and(my_slot >= thin_low, my_slot < thin_high))
    my_wide = jnp.logical_and(keeps, jnp.logical_not(my_thin))
    lane = lax.broadcasted_iota(jnp.int32, (1, half), 1)

    def back_copy(turn, quad, slot, peer, tiles):
        return pltpu.make_async_remote_copy(
            src_ref=back_sent.at[quad, slot, pl.ds(0, tiles)], dst_ref=back_came.at[quad, me, pl.ds(0, tiles)],
            send_sem=back_send_sem.at[turn], recv_sem=back_sem.at[quads * turn + quad],
            device_id={"fft": peer}, device_id_type=MESH,
        )

    def turn_lanes(x, amount):
        return pltpu.roll(x, amount, x.ndim - 1)

    def packed(block):
        a, b, c, d = (block[k] for k in range(4))
        left = lane < half // 2
        ends = jnp.where(
            left,
            jnp.where(lane < half // 4, turn_lanes(a, half // 2), turn_lanes(b, 3 * half // 4)),
            jnp.where(lane < 3 * half // 4, c, turn_lanes(d, half // 4)),
        )
        return jnp.stack(
            [
                jnp.where(left, a, turn_lanes(b, half // 2)),
                jnp.where(left, c, turn_lanes(d, half // 2)),
                ends,
            ]
        )

    def unpacked(quad):
        first, second, ends = (
            back_came[quad, :, k].reshape(2 * length, half) for k in range(3)
        )
        left = lane < half // 2
        return (
            jnp.where(left, first, turn_lanes(ends, half // 2)),
            jnp.where(left, turn_lanes(first, half // 2), turn_lanes(ends, half // 4)),
            jnp.where(left, second, ends),
            jnp.where(left, turn_lanes(second, half // 2), turn_lanes(ends, 3 * half // 4)),
        )

    def send_rows(turn):
        def one(at, _):
            quad, slot = at // len(kept), lax.rem(at, len(kept))
            peer = jnp.where(slot < low, slot, slot + gap)
            start = pl.multiple_of(slot * 2 * rows + quad * 8, 8)
            block = jnp.swapaxes(flat[:, pl.ds(start, 8), :], 0, 1).reshape(4, 2 * planes, half)
            tiles = packed(block).astype(BF16)
            back_sent[quad, slot] = tiles

            @pl.when(peer == me)
            def _():
                back_came[quad, me] = tiles

            thin = jnp.logical_and(slot >= thin_low, slot < thin_high)

            @pl.when(jnp.logical_and(peer != me, thin))
            def _():
                back_copy(turn, quad, slot, peer, 2).start()

            @pl.when(jnp.logical_and(peer != me, jnp.logical_not(thin)))
            def _():
                back_copy(turn, quad, slot, peer, 3).start()

            return 0

        lax.fori_loop(0, quads * len(kept), one, 0)

    def wait_rows_sent(turn):
        thin_count = thin_high - thin_low
        wide_count = len(kept) - thin_count
        for quad in range(quads):
            for tiles, count, own in ((2, thin_count, my_thin), (3, wide_count, my_wide)):
                @pl.when(own)
                def _():
                    sent_tiles(turn, tiles, count - 1).wait_send()

                @pl.when(jnp.logical_not(own))
                def _():
                    sent_tiles(turn, tiles, count).wait_send()

    def sent_tiles(turn, tiles, count):
        piece = back_sent.at[0, pl.ds(0, count), pl.ds(0, tiles)]
        return pltpu.make_async_remote_copy(
            src_ref=piece, dst_ref=piece, send_sem=back_send_sem.at[turn],
            recv_sem=back_sem.at[quads * turn], device_id={"fft": me}, device_id_type=MESH,
        )

    def wait_rows(turn, quad):
        for tiles, own in ((2, my_thin), (3, my_wide)):
            @pl.when(own)
            def _():
                piece = back_came.at[0, pl.ds(0, parts - 1), pl.ds(0, tiles)]
                pltpu.make_async_remote_copy(
                    src_ref=piece, dst_ref=piece, send_sem=back_send_sem.at[turn],
                    recv_sem=back_sem.at[quads * turn + quad], device_id={"fft": me}, device_id_type=MESH,
                ).wait_recv()

    def tendency(quad, use):
        held = unpacked(quad)
        for pair in (0, 1):
            done = dot(z_fwd[...], jnp.concatenate(held[2 * pair : 2 * pair + 2], axis=1))
            for side in (0, 1):
                use(4 * quad + 2 * pair + side, done[:, side * half : (side + 1) * half])

    def speeds_copy(k, block, peer, at=None):
        ref = speeds.at[block] if at is None else speeds.at[block, :, pl.ds(at, planes // 2)]
        return pltpu.make_async_remote_copy(
            src_ref=ref, dst_ref=ref, send_sem=vel_send.at[k], recv_sem=vel_recv.at[k],
            device_id={"scal": peer}, device_id_type=MESH,
        )

    @pl.when(jnp.logical_not(my_wide))
    def _():
        back_came[...] = jnp.zeros_like(back_came)

    own_speeds.wait()
    send_planes(0)
    speeds_copy(0, mine, far).wait_send()
    speeds_copy(0, far, far).wait_recv()
    for k, peer in ((1, up), (3, down)):
        speeds_copy(k, mine, peer).start()
        speeds_copy(k + 1, far, peer).start()

    def half_one(chunk, peak):
        wait_planes(0, chunk)
        gradient_pair(chunk)
        return peak_of(2 * chunk + 1, peak_of(2 * chunk, peak))

    peak = jnp.zeros((8, length), F32)
    peak = lax.fori_loop(0, pairs // 2, half_one, peak)
    cut = planes // 2
    speeds_copy(1, down, up).wait_recv()
    speeds_copy(2, far_down, up).wait_recv()
    speeds_copy(5, down, up, 0).start()
    speeds_copy(6, far_down, up, 0).start()
    speeds_copy(3, up, down).wait_recv()
    speeds_copy(4, far_up, down).wait_recv()
    speeds_copy(7, up, down, cut).start()
    speeds_copy(8, far_up, down, cut).start()

    def half_two(chunk, peak):
        peak = half_one(chunk, peak)
        late = chunk == pairs - 2

        @pl.when(late)
        def _():
            for k, peer in ((1, up), (3, down)):
                speeds_copy(k, mine, peer).wait_send()
                speeds_copy(k + 1, far, peer).wait_send()
            speeds_copy(5, across, up, 0).wait()
            speeds_copy(6, far_across, up, 0).wait()
            speeds_copy(7, across, down, cut).wait()
            speeds_copy(8, far_across, down, cut).wait()

        @pl.loop(jnp.where(late, 0, chunk), chunk + 1)
        def _(k):
            forward_pair(k)

        return peak

    peak = lax.fori_loop(pairs // 2, pairs, half_two, peak)

    peak = jnp.maximum(peak[:, :half], peak[:, half:])
    stats[me] = jnp.concatenate(
        [
            jnp.sum(variance_part, axis=0, keepdims=True),
            jnp.sum(grad_part, axis=0, keepdims=True),
            jnp.max(peak, axis=0, keepdims=True),
            jnp.zeros((5, half), F32),
        ],
        axis=0,
    )

    @pl.loop(1, parts)
    def _(k):
        pltpu.make_async_remote_copy(
            src_ref=stats.at[me], dst_ref=stats.at[me], send_sem=stat_send_sem, recv_sem=stat_sem,
            device_id={"fft": lax.rem(me + k, parts)}, device_id_type=MESH,
        ).start()

    send_rows(0)
    wait_sent(0)
    everyone = stats.at[pl.ds(0, parts - 1)]
    stat_wait = pltpu.make_async_remote_copy(
        src_ref=everyone, dst_ref=everyone, send_sem=stat_send_sem, recv_sem=stat_sem,
        device_id={"fft": me}, device_id_type=MESH,
    )
    stat_wait.wait_send()
    stat_wait.wait_recv()
    collected = stats[...]
    variance = jnp.sum(jnp.sum(collected[:, 0], axis=0, keepdims=True), axis=1, keepdims=True) / cell_count
    mean_grad = jnp.sum(jnp.sum(collected[:, 1], axis=0, keepdims=True), axis=1, keepdims=True) / cell_count
    largest = jnp.max(jnp.max(collected[:, 2], axis=0, keepdims=True), axis=1, keepdims=True)
    count = table.shape[1]
    match = lax.broadcasted_iota(jnp.int32, (1, count), 1) == species[0]
    base = jnp.sum(jnp.where(match, table[...], 0.0), axis=1, keepdims=True)
    kappa = base * jnp.sqrt(largest) * jnp.sqrt(variance) / (mean_grad + 1e-06)
    kappa_out[...] = jnp.broadcast_to(kappa, kappa_out.shape)
    limit = bound[0].astype(F32)
    limit = limit * limit

    def to_middle(row, done):
        ksquare = square(row)
        keep = ksquare <= limit
        factor = jnp.exp(-kappa * ksquare * step_size)
        moved = []
        for part in (0, 1):
            start = state[part, row]
            rate = jnp.where(keep, -done[part * length : (part + 1) * length], 0.0)
            moved.append(factor * (start + step_size * rate))
            out[part, row] = factor * start + 0.5 * step_size * (factor * rate)
        put_spectrum(row, *moved)

    @pl.loop(0, quads)
    def _(quad):
        wait_rows(0, quad)
        tendency(quad, to_middle)

    send_planes(1)

    @pl.loop(0, pairs)
    def _(chunk):
        wait_planes(1, chunk)
        gradient_pair(chunk)
        forward_pair(chunk)

    wait_rows_sent(0)
    send_rows(1)
    wait_sent(1)

    def to_end(row, done):
        keep = square(row) <= limit
        for part in (0, 1):
            rate = jnp.where(keep, -done[part * length : (part + 1) * length], 0.0)
            out[part, row] = out[part, row] + 0.5 * step_size * rate

    @pl.loop(0, quads)
    def _(quad):
        wait_rows(1, quad)
        tendency(quad, to_end)

    wait_rows_sent(1)


def body(parts, groups, scalar_state, velocity, species, kappa_table, dealias_bound):
    _, _, rows, length, half = scalar_state.shape
    planes = length // parts
    kept = kept_slabs(length, parts)
    tables = build_tables(length, parts)
    near = groups // 2
    chunk_rows = velocity.shape[2]
    vmem = pl.BlockSpec(memory_space=pltpu.VMEM)
    smem = pl.BlockSpec(memory_space=pltpu.SMEM)
    hbm = pl.BlockSpec(memory_space=pl.ANY)
    DMA = pltpu.SemaphoreType.DMA
    new_state, kappa = pl.pallas_call(
        functools.partial(kernel, parts, groups, near),
        out_shape=(
            jax.ShapeDtypeStruct((2, rows, length, half), F32),
            jax.ShapeDtypeStruct((8, half), F32),
        ),
        in_specs=[vmem, hbm, smem, vmem, smem] + [vmem] * len(tables),
        out_specs=(vmem, vmem),
        scratch_shapes=[
            pltpu.VMEM((rows, 2 * length, 2 * half), BF16),
            pltpu.VMEM((rows, 16 * planes, 2 * half), F32),
            pltpu.VMEM((parts, planes, 2 * rows, 2 * half), BF16),
            pltpu.VMEM((planes, parts, 2 * rows, 2 * half), BF16),
            pltpu.VMEM((groups, 3, planes, chunk_rows, length), BF16),
            pltpu.VMEM((3, planes, length, length), F32),
            pltpu.VMEM((2 * length, 2 * half), BF16),
            pltpu.VMEM((planes, len(kept) * 2 * rows, half), F32),
            pltpu.VMEM((rows // 4, len(kept), 3, 2 * planes, half), BF16),
            pltpu.VMEM((rows // 4, parts, 3, 2 * planes, half), BF16),
            pltpu.VMEM((parts, 8, half), F32),
            DMA((2,)),
            DMA((planes,)),
            DMA((2,)),
            DMA((rows // 2,)),
            DMA,
            DMA,
            DMA,
            DMA((9,)),
            DMA((9,)),
        ],
        compiler_params=pltpu.CompilerParams(
            collective_id=0, has_side_effects=True, vmem_limit_bytes=60 * 1024 * 1024
        ),
    )(scalar_state[0], velocity, species, kappa_table[None, :], dealias_bound, *tables)
    return new_state[None], kappa[0, :1]


def solution(mesh):
    parts, groups = mesh.shape["fft"], mesh.shape["scal"]
    placed = (
        P("scal", None, "fft", None, None),
        P(None, "fft", "scal", None),
        P("scal"),
        P(),
        P("scal"),
    )
    return jax.shard_map(
        functools.partial(body, parts, groups),
        mesh=mesh,
        in_specs=placed,
        out_specs=(P("scal", None, "fft", None, None), P("scal")),
        check_vma=False,
    )
```

```python
import functools
import math

import jax
import jax.numpy as jnp
import numpy as np
from jax import lax
from jax.experimental import pallas as pl
from jax.experimental.pallas import tpu as pltpu
from jax.sharding import PartitionSpec as P

MESH = pl.DeviceIdType.MESH
cfl_number = 0.2
LARGEST_BOUND = 85
F32, BF16 = jnp.float32, jnp.bfloat16


def base_tables(length):
    index = np.arange(length)
    angles = (index[:, None] * index[None, :] % length).astype(np.float32) * np.float32(2.0 * math.pi / length)
    norming = np.float32(1.0 / math.sqrt(length))
    cos = (np.cos(angles).astype(np.float32) * norming).astype(np.float32)
    sin = (np.sin(angles).astype(np.float32) * norming).astype(np.float32)
    return cos, sin


def kept_slabs(length, parts):
    rows = length // parts
    signed = np.where(np.arange(length) < length // 2, np.arange(length), np.arange(length) - length)
    return [d for d in range(parts) if np.min(np.abs(signed[d * rows : (d + 1) * rows])) <= LARGEST_BOUND]


def narrow_slots(length, parts, half):
    rows = length // parts
    thin = []
    for slot, d in enumerate(kept_slabs(length, parts)):
        ky = np.arange(d * rows, (d + 1) * rows)
        least = np.min(np.abs(np.where(ky < length // 2, ky, ky - length)))
        if LARGEST_BOUND**2 - least**2 < (half // 2) ** 2:
            thin.append(slot)
    assert thin == list(range(thin[0], thin[-1] + 1))
    return thin[0], thin[-1] + 1


def batch_order(parts):
    ring = parts // 4
    return [
        column * (parts // 2) + (place + side * (ring // 2)) * 2 + core
        for place in range(ring // 2) for column in (0, 1) for side in (0, 1) for core in (0, 1)
    ]


def build_tables(length, parts):
    cos, sin = base_tables(length)
    half, rows = length // 2, length // parts
    weight = np.where(np.arange(half) == 0, 1.0, 2.0).astype(np.float32)[:, None]
    real = np.stack([cos, -sin], axis=1)
    imag = np.stack([sin, cos], axis=1)
    inverse = np.stack([real, imag]).transpose(0, 3, 2, 1)
    turned = np.stack([np.stack([-sin, -cos], 1), np.stack([cos, -sin], 1)]).transpose(0, 3, 2, 1)
    forward = np.stack([np.stack([cos, sin], 1), np.stack([-sin, cos], 1)]).transpose(0, 3, 2, 1)
    size = 2 * length

    def slab_columns(table):
        return table.reshape(size, 2, parts, rows).transpose(0, 2, 1, 3).reshape(size, size)

    def slab_rows(table):
        return table.transpose(1, 0, 2, 3).reshape(size, size)

    kept = kept_slabs(length, parts)
    z_inv = slab_rows(inverse).reshape(parts, 2 * rows, size)[batch_order(parts)].reshape(size, size)
    y_inv = slab_columns(inverse)
    y_inv_turned = slab_columns(turned)
    y_fwd = slab_rows(forward).reshape(parts, 2 * rows, size)[kept].reshape(-1, size)
    z_fwd = slab_columns(forward)
    x_inv = np.concatenate([cos[:half] * weight, -(sin[:half] * weight)], axis=0)
    x_fwd = np.concatenate([cos[:, :half], -sin[:, :half]], axis=1)
    listed = (z_inv, y_inv, y_inv_turned, y_fwd, z_fwd, x_inv, x_fwd)
    return tuple(jnp.asarray(t.astype(np.float32)).astype(BF16) for t in listed)


def dot(a, b):
    return jnp.dot(a, b, preferred_element_type=F32)


def signed_of(index, length):
    return jnp.where(index < length // 2, index, index - length).astype(F32)


def kernel(
    parts, groups, near,
    state, velocity, species, table, bound,
    z_inv, *rest,
):
    (
        *far_tables, out, kappa_out,
        y_inv, y_inv_turned, y_fwd, z_fwd, x_inv, x_fwd, table_sem, spec, work, sent, came, speeds, grads, lines, flat, back_sent, back_came, stats,
        send_sem, came_sem, back_send_sem, back_sem, stat_send_sem, stat_sem, vel_sem, vel_send, vel_recv,
    ) = rest
    rows, length, half = state.shape[1], state.shape[2], state.shape[3]
    kept = kept_slabs(length, parts)
    low = sum(1 for d in kept if d < parts // 2)
    gap = parts - len(kept)
    planes = length // parts
    pairs = planes // 2
    step_size = cfl_number * 2.0 * math.pi / length
    cell_count = float(length) ** 3
    me = lax.axis_index("fft")
    mine = lax.axis_index("scal")
    far = lax.rem(mine + groups // 2, groups)
    upper = (mine // near) * near
    up = upper + lax.rem(mine + 1, near)
    down = upper + lax.rem(mine + near - 1, near)
    far_up, far_down = lax.rem(up + groups // 2, groups), lax.rem(down + groups // 2, groups)
    across = upper + lax.rem(mine + 2, near)
    far_across = lax.rem(across + groups // 2, groups)

    barrier = pltpu.get_barrier_semaphore()

    @pl.loop(1, parts)
    def _(k):
        pl.semaphore_signal(barrier, inc=1, device_id={"fft": lax.rem(me + k, parts)}, device_id_type=MESH)

    for peer in (far, up, down):
        pl.semaphore_signal(barrier, inc=1, device_id={"scal": peer}, device_id_type=MESH)

    own_speeds = pltpu.make_async_copy(velocity, speeds.at[mine], vel_sem)
    own_speeds.start()
    table_copies = [
        pltpu.make_async_copy(src, dst, table_sem.at[k])
        for k, (src, dst) in enumerate(zip(far_tables, (y_inv, y_inv_turned, y_fwd, z_fwd, x_inv, x_fwd)))
    ]
    for copy in table_copies:
        copy.start()

    kz = signed_of(lax.broadcasted_iota(jnp.int32, (length, 1), 0), length)
    kx_index = lax.broadcasted_iota(jnp.int32, (1, half), 1)
    kx = kx_index.astype(F32)
    weight = jnp.where(kx_index == 0, 1.0, 2.0).astype(F32)

    def square(row):
        ky = signed_of(me * rows + row, length)
        return kx * kx + ky * ky + kz * kz

    def put_spectrum(row, real, imag):
        here = pl.ds(pl.multiple_of(row * 2 * half, 2 * half), half)
        there = pl.ds(pl.multiple_of(row * 2 * half + half, half), half)
        spec[:length, here] = real.astype(BF16)
        spec[length:, here] = imag.astype(BF16)
        spec[:length, there] = (-kz * imag).astype(BF16)
        spec[length:, there] = (kz * real).astype(BF16)

    def fold(x):
        return jnp.sum(x.reshape(length // 8, 8, half), axis=0)

    @pl.loop(0, rows)
    def _(row):
        put_spectrum(row, state[0, row], state[1, row])

    def row_energy(row, total):
        real, imag = state[0, row], state[1, row]
        energy = weight * (real * real + imag * imag)
        return total[0] + fold(energy), total[1] + fold(square(row) * energy)

    batch = 8
    batches = parts // batch
    batch_rows = batch * 2 * planes
    ring = parts // 4
    my_place = lax.rem(me // 2, ring)

    def slab_at(column, place, core):
        return column * (parts // 2) + place * 2 + core

    def peer_in_batch(which, j):
        return slab_at(j // 4, which + lax.rem(j // 2, 2) * (ring // 2), lax.rem(j, 2))

    def peer_in_turn(i):
        q = i // 4
        step = jnp.where(lax.rem(q, 2) == 1, (q + 1) // 2, ring - q // 2)
        column = lax.rem(me // (parts // 2) + lax.rem(i // 2, 2), 2)
        return slab_at(column, lax.rem(my_place + step, ring), lax.rem(me + i, 2))

    def came_copy(turn, chunk, peer):
        return pltpu.make_async_remote_copy(
            src_ref=sent.at[peer, pl.ds(2 * chunk, 2)],
            dst_ref=came.at[pl.ds(2 * chunk, 2), me],
            send_sem=send_sem.at[turn],
            recv_sem=came_sem.at[turn * pairs + chunk],
            device_id={"fft": peer},
            device_id_type=MESH,
        )

    def send_planes(turn):
        def one_batch(k, _):
            which = lax.rem(my_place + batches // 2 + k, batches)
            at = pl.multiple_of(which * batch_rows, batch_rows)
            work[...] = dot(z_inv[pl.ds(at, batch_rows), :], spec[...])
            for j in range(batch):
                peer = peer_in_batch(which, j)
                strip = work[j * 2 * planes : (j + 1) * 2 * planes, :]
                block = jnp.stack([strip[:, row * 2 * half : (row + 1) * 2 * half] for row in range(rows)])
                turned = jnp.swapaxes(block, 0, 1).reshape(planes, 2 * rows, 2 * half).astype(BF16)
                sent[peer] = turned

            if turn == 0:
                @pl.when(k == 0)
                def _():
                    pl.semaphore_wait(barrier, parts - 1 + 3)
                    speeds_copy(0, mine, far).start()
                    speeds_copy(1, mine, up).start()
                    speeds_copy(3, mine, down).start()

            @pl.loop(0, batch)
            def _(j):
                peer = peer_in_batch(which, j)

                @pl.when(peer != me)
                def _():
                    came_copy(turn, 0, peer).start()

            return 0

        lax.fori_loop(0, parts // batch, one_batch, 0)
        came[:, pl.ds(me, 1)] = sent[me][:, None]

        @pl.loop(1, pairs)
        def _(chunk):
            @pl.loop(1, parts)
            def _(i):
                came_copy(turn, chunk, peer_in_turn(i)).start()

    def wait_planes(turn, chunk):
        piece = sent.at[pl.ds(0, parts - 1), pl.ds(0, 2)]
        pltpu.make_async_remote_copy(
            src_ref=piece, dst_ref=piece, send_sem=send_sem.at[turn],
            recv_sem=came_sem.at[turn * pairs + chunk], device_id={"fft": me}, device_id_type=MESH,
        ).wait_recv()

    def wait_sent(turn):
        piece = sent.at[pl.ds(0, parts - 1)]
        pltpu.make_async_remote_copy(
            src_ref=piece, dst_ref=piece, send_sem=send_sem.at[turn],
            recv_sem=came_sem.at[turn * pairs], device_id={"fft": me}, device_id_type=MESH,
        ).wait_send()

    ky_row = lax.broadcasted_iota(jnp.int32, (2 * length, 1), 0)
    ky_row = signed_of((ky_row // (2 * rows)) * rows + lax.rem(ky_row, rows), length).astype(BF16)
    kx_low = kx.astype(BF16)

    def to_grid(field, plane, real, imag):
        halves = jnp.concatenate([real, imag], axis=1).astype(BF16)
        grads[field, plane] = dot(halves, x_inv[...])

    def gradient_pair(chunk):
        last = []
        for side in (0, 1):
            plane = 2 * chunk + side
            both = came[plane].reshape(2 * length, 2 * half)
            whole, deriv = both[:, :half], both[:, half:]
            last.append(deriv)
            scaled = jnp.concatenate([whole * kx_low, whole * ky_row], axis=1)
            done = dot(y_inv_turned[...], scaled)
            to_grid(0, plane, done[:length, :half], done[length:, :half])
            to_grid(1, plane, done[:length, half:], done[length:, half:])
        done = dot(y_inv[...], jnp.concatenate(last, axis=1))
        to_grid(2, 2 * chunk, done[:length, :half], done[length:, :half])
        to_grid(2, 2 * chunk + 1, done[:length, half:], done[length:, half:])

    def peak_of(plane, peak):
        gx, gy, gz = grads[0, plane], grads[1, plane], grads[2, plane]
        size = gx * gx + gy * gy + gz * gz
        return jnp.maximum(peak, jnp.max(size.reshape(-1, 8, length), axis=0))

    def forward_pair(chunk):
        for side in (0, 1):
            plane = 2 * chunk + side
            total = speeds[:, 0, plane].reshape(length, length).astype(F32) * grads[0, plane]
            total = total + speeds[:, 1, plane].reshape(length, length).astype(F32) * grads[1, plane]
            total = total + speeds[:, 2, plane].reshape(length, length).astype(F32) * grads[2, plane]
            part = dot(total.astype(BF16), x_fwd[...]).astype(BF16)
            lines[:length, side * half : (side + 1) * half] = part[:, :half]
            lines[length:, side * half : (side + 1) * half] = part[:, half:]
        done = dot(y_fwd[...], lines[...])
        flat[2 * chunk] = done[:, :half]
        flat[2 * chunk + 1] = done[:, half:]

    quads = rows // 4
    keeps = jnp.logical_or(me < low, me >= low + gap)
    my_slot = jnp.where(me < low, me, me - gap)
    thin_low, thin_high = narrow_slots(length, parts, half)
    my_thin = jnp.logical_and(keeps, jnp.logical_and(my_slot >= thin_low, my_slot < thin_high))
    my_wide = jnp.logical_and(keeps, jnp.logical_not(my_thin))
    lane = lax.broadcasted_iota(jnp.int32, (1, half), 1)

    def back_copy(turn, quad, slot, peer, tiles):
        return pltpu.make_async_remote_copy(
            src_ref=back_sent.at[quad, slot, pl.ds(0, tiles)], dst_ref=back_came.at[quad, me, pl.ds(0, tiles)],
            send_sem=back_send_sem.at[turn], recv_sem=back_sem.at[quads * turn + quad],
            device_id={"fft": peer}, device_id_type=MESH,
        )

    def turn_lanes(x, amount):
        return pltpu.roll(x, amount, x.ndim - 1)

    def packed(block):
        a, b, c, d = (block[k] for k in range(4))
        left = lane < half // 2
        ends = jnp.where(
            left,
            jnp.where(lane < half // 4, turn_lanes(a, half // 2), turn_lanes(b, 3 * half // 4)),
            jnp.where(lane < 3 * half // 4, c, turn_lanes(d, half // 4)),
        )
        return jnp.stack(
            [
                jnp.where(left, a, turn_lanes(b, half // 2)),
                jnp.where(left, c, turn_lanes(d, half // 2)),
                ends,
            ]
        )

    def unpacked(quad):
        first, second, ends = (
            back_came[quad, :, k].reshape(2 * length, half) for k in range(3)
        )
        left = lane < half // 2
        return (
            jnp.where(left, first, turn_lanes(ends, half // 2)),
            jnp.where(left, turn_lanes(first, half // 2), turn_lanes(ends, half // 4)),
            jnp.where(left, second, ends),
            jnp.where(left, turn_lanes(second, half // 2), turn_lanes(ends, 3 * half // 4)),
        )

    thin_count = thin_high - thin_low
    wide_count = len(kept) - thin_count

    def start_rows(turn, quad, tiles, count, slot_of):
        @pl.loop(0, count)
        def _(i):
            away = jnp.where(lax.rem(i, 2) == 1, (i + 1) // 2, count - i // 2)
            slot = slot_of(lax.rem(me * count // parts + away, count))
            peer = jnp.where(slot < low, slot, slot + gap)

            @pl.when(peer != me)
            def _():
                back_copy(turn, quad, slot, peer, tiles).start()

    def send_rows(turn):
        @pl.loop(0, quads)
        def _(quad):
            for slot in range(len(kept)):
                start = pl.multiple_of(slot * 2 * rows + quad * 8, 8)
                block = jnp.swapaxes(flat[:, pl.ds(start, 8), :], 0, 1).reshape(4, 2 * planes, half)
                back_sent[quad, slot] = packed(block).astype(BF16)
            start_rows(turn, quad, 3, wide_count, lambda k: jnp.where(k < thin_low, k, k + thin_count))
            start_rows(turn, quad, 2, thin_count, lambda k: k + thin_low)

            @pl.when(keeps)
            def _():
                back_came[quad, me] = back_sent[quad, my_slot]

    def wait_rows_sent(turn):
        for quad in range(quads):
            for tiles, count, own in ((2, thin_count, my_thin), (3, wide_count, my_wide)):
                @pl.when(own)
                def _():
                    sent_tiles(turn, tiles, count - 1).wait_send()

                @pl.when(jnp.logical_not(own))
                def _():
                    sent_tiles(turn, tiles, count).wait_send()

    def sent_tiles(turn, tiles, count):
        piece = back_sent.at[0, pl.ds(0, count), pl.ds(0, tiles)]
        return pltpu.make_async_remote_copy(
            src_ref=piece, dst_ref=piece, send_sem=back_send_sem.at[turn],
            recv_sem=back_sem.at[quads * turn], device_id={"fft": me}, device_id_type=MESH,
        )

    def wait_rows(turn, quad):
        for tiles, own in ((2, my_thin), (3, my_wide)):
            @pl.when(own)
            def _():
                piece = back_came.at[0, pl.ds(0, parts - 1), pl.ds(0, tiles)]
                pltpu.make_async_remote_copy(
                    src_ref=piece, dst_ref=piece, send_sem=back_send_sem.at[turn],
                    recv_sem=back_sem.at[quads * turn + quad], device_id={"fft": me}, device_id_type=MESH,
                ).wait_recv()

    def tendency(quad, use):
        held = unpacked(quad)
        for pair in (0, 1):
            done = dot(z_fwd[...], jnp.concatenate(held[2 * pair : 2 * pair + 2], axis=1))
            for side in (0, 1):
                use(4 * quad + 2 * pair + side, done[:, side * half : (side + 1) * half])

    def speeds_copy(k, block, peer, at=None):
        ref = speeds.at[block] if at is None else speeds.at[block, :, pl.ds(at, planes // 2)]
        return pltpu.make_async_remote_copy(
            src_ref=ref, dst_ref=ref, send_sem=vel_send.at[k], recv_sem=vel_recv.at[k],
            device_id={"scal": peer}, device_id_type=MESH,
        )

    @pl.when(jnp.logical_not(my_wide))
    def _():
        back_came[...] = jnp.zeros_like(back_came)

    own_speeds.wait()
    send_planes(0)
    zero = jnp.zeros((8, half), F32)
    variance_part, grad_part = lax.fori_loop(0, rows, row_energy, (zero, zero))
    for copy in table_copies:
        copy.wait()
    cut = planes // 2
    speeds_copy(1, down, up).wait_recv()
    speeds_copy(5, down, up, 0).start()
    speeds_copy(3, up, down).wait_recv()
    speeds_copy(7, up, down, cut).start()
    speeds_copy(0, far, far).wait_recv()
    speeds_copy(2, far, up).start()
    speeds_copy(4, far, down).start()

    def half_one(chunk, peak):
        wait_planes(0, chunk)
        gradient_pair(chunk)
        return peak_of(2 * chunk + 1, peak_of(2 * chunk, peak))

    peak = jnp.zeros((8, length), F32)
    peak = lax.fori_loop(0, pairs // 2, half_one, peak)
    speeds_copy(2, far_down, up).wait_recv()
    speeds_copy(6, far_down, up, 0).start()
    speeds_copy(4, far_up, down).wait_recv()
    speeds_copy(8, far_up, down, cut).start()

    def half_two(chunk, peak):
        peak = half_one(chunk, peak)
        late = chunk == pairs - 2

        @pl.when(late)
        def _():
            speeds_copy(0, mine, far).wait_send()
            for k, peer in ((1, up), (3, down)):
                speeds_copy(k, mine, peer).wait_send()
                speeds_copy(k + 1, far, peer).wait_send()
            speeds_copy(5, across, up, 0).wait()
            speeds_copy(6, far_across, up, 0).wait()
            speeds_copy(7, across, down, cut).wait()
            speeds_copy(8, far_across, down, cut).wait()

        @pl.loop(jnp.where(late, 0, chunk), chunk + 1)
        def _(k):
            forward_pair(k)

        return peak

    peak = lax.fori_loop(pairs // 2, pairs, half_two, peak)

    def whole(reduce, x):
        return reduce(reduce(x, axis=0, keepdims=True), axis=1, keepdims=True)

    stats[pl.ds(me, 1)] = jnp.where(
        lane == 0,
        whole(jnp.sum, variance_part),
        jnp.where(lane == 1, whole(jnp.sum, grad_part), whole(jnp.max, peak)),
    )[None]

    @pl.loop(1, parts)
    def _(k):
        pltpu.make_async_remote_copy(
            src_ref=stats.at[me], dst_ref=stats.at[me], send_sem=stat_send_sem, recv_sem=stat_sem,
            device_id={"fft": lax.rem(me + k, parts)}, device_id_type=MESH,
        ).start()

    send_rows(0)
    wait_sent(0)
    everyone = stats.at[pl.ds(0, parts - 1)]
    stat_wait = pltpu.make_async_remote_copy(
        src_ref=everyone, dst_ref=everyone, send_sem=stat_send_sem, recv_sem=stat_sem,
        device_id={"fft": me}, device_id_type=MESH,
    )
    stat_wait.wait_send()
    stat_wait.wait_recv()
    collected = stats[...].reshape(parts, half)
    sums = jnp.sum(collected, axis=0, keepdims=True)
    variance = sums[:, :1] / cell_count
    mean_grad = sums[:, 1:2] / cell_count
    largest = jnp.max(collected, axis=0, keepdims=True)[:, 2:3]
    count = table.shape[1]
    match = lax.broadcasted_iota(jnp.int32, (1, count), 1) == species[0]
    base = jnp.sum(jnp.where(match, table[...], 0.0), axis=1, keepdims=True)
    kappa = base * jnp.sqrt(largest) * jnp.sqrt(variance) / (mean_grad + 1e-06)
    kappa_out[...] = jnp.broadcast_to(kappa, kappa_out.shape)
    limit = bound[0].astype(F32)
    limit = limit * limit

    def to_middle(row, done):
        ksquare = square(row)
        keep = ksquare <= limit
        factor = jnp.exp(-kappa * ksquare * step_size)
        moved = []
        for part in (0, 1):
            start = state[part, row]
            rate = jnp.where(keep, -done[part * length : (part + 1) * length], 0.0)
            moved.append(factor * (start + step_size * rate))
            out[part, row] = factor * start + 0.5 * step_size * (factor * rate)
        put_spectrum(row, *moved)

    @pl.loop(0, quads)
    def _(quad):
        wait_rows(0, quad)
        tendency(quad, to_middle)

    send_planes(1)

    @pl.loop(0, pairs)
    def _(chunk):
        wait_planes(1, chunk)
        gradient_pair(chunk)
        forward_pair(chunk)

    wait_rows_sent(0)
    send_rows(1)
    wait_sent(1)

    def to_end(row, done):
        keep = square(row) <= limit
        for part in (0, 1):
            rate = jnp.where(keep, -done[part * length : (part + 1) * length], 0.0)
            out[part, row] = out[part, row] + 0.5 * step_size * rate

    @pl.loop(0, quads)
    def _(quad):
        wait_rows(1, quad)
        tendency(quad, to_end)


    wait_rows_sent(1)


def body(parts, groups, scalar_state, velocity, species, kappa_table, dealias_bound):
    _, _, rows, length, half = scalar_state.shape
    planes = length // parts
    kept = kept_slabs(length, parts)
    tables = build_tables(length, parts)
    near = groups // 2
    chunk_rows = velocity.shape[2]
    vmem = pl.BlockSpec(memory_space=pltpu.VMEM)
    smem = pl.BlockSpec(memory_space=pltpu.SMEM)
    hbm = pl.BlockSpec(memory_space=pl.ANY)
    DMA = pltpu.SemaphoreType.DMA
    new_state, kappa = pl.pallas_call(
        functools.partial(kernel, parts, groups, near),
        out_shape=(pltpu.VMEM((2, rows, length, half), F32), pltpu.VMEM((8, half), F32)),
        in_specs=[vmem, hbm, smem, vmem, smem, vmem] + [hbm] * (len(tables) - 1),
        out_specs=(vmem, vmem),
        scratch_shapes=[
            *(pltpu.VMEM(t.shape, t.dtype) for t in tables[1:]),
            DMA((len(tables) - 1,)),
            pltpu.VMEM((2 * length, rows * 2 * half), BF16),
            pltpu.VMEM((16 * planes, rows * 2 * half), F32),
            pltpu.VMEM((parts, planes, 2 * rows, 2 * half), BF16),
            pltpu.VMEM((planes, parts, 2 * rows, 2 * half), BF16),
            pltpu.VMEM((groups, 3, planes, chunk_rows, length), BF16),
            pltpu.VMEM((3, planes, length, length), F32),
            pltpu.VMEM((2 * length, 2 * half), BF16),
            pltpu.VMEM((planes, len(kept) * 2 * rows, half), F32),
            pltpu.VMEM((rows // 4, len(kept), 3, 2 * planes, half), BF16),
            pltpu.VMEM((rows // 4, parts, 3, 2 * planes, half), BF16),
            pltpu.VMEM((parts, 1, half), F32),
            DMA((2,)),
            DMA((planes,)),
            DMA((2,)),
            DMA((rows // 2,)),
            DMA,
            DMA,
            DMA,
            DMA((9,)),
            DMA((9,)),
        ],
        compiler_params=pltpu.CompilerParams(
            collective_id=0, has_side_effects=True, vmem_limit_bytes=60 * 1024 * 1024
        ),
    )(scalar_state[0], velocity, species, kappa_table[None, :], dealias_bound, *tables)
    return new_state[None], kappa[0, :1]


def solution(mesh):
    parts, groups = mesh.shape["fft"], mesh.shape["scal"]
    placed = (
        P("scal", None, "fft", None, None),
        P(None, "fft", "scal", None),
        P("scal"),
        P(),
        P("scal"),
    )
    return jax.shard_map(
        functools.partial(body, parts, groups),
        mesh=mesh,
        in_specs=placed,
        out_specs=(P("scal", None, "fft", None, None), P("scal")),
        check_vma=False,
    )
```

```python
import functools
import math

import jax
import jax.numpy as jnp
import numpy as np
from jax import lax
from jax.experimental import pallas as pl
from jax.experimental.pallas import tpu as pltpu
from jax.sharding import PartitionSpec as P

MESH = pl.DeviceIdType.MESH
cfl_number = 0.2
LARGEST_BOUND = 85
F32, BF16 = jnp.float32, jnp.bfloat16


def base_tables(length):
    index = np.arange(length)
    angles = (index[:, None] * index[None, :] % length).astype(np.float32) * np.float32(2.0 * math.pi / length)
    norming = np.float32(1.0 / math.sqrt(length))
    cos = (np.cos(angles).astype(np.float32) * norming).astype(np.float32)
    sin = (np.sin(angles).astype(np.float32) * norming).astype(np.float32)
    return cos, sin


def kept_slabs(length, parts):
    rows = length // parts
    signed = np.where(np.arange(length) < length // 2, np.arange(length), np.arange(length) - length)
    return [d for d in range(parts) if np.min(np.abs(signed[d * rows : (d + 1) * rows])) <= LARGEST_BOUND]


def narrow_slots(length, parts, half):
    rows = length // parts
    thin = []
    for slot, d in enumerate(kept_slabs(length, parts)):
        ky = np.arange(d * rows, (d + 1) * rows)
        least = np.min(np.abs(np.where(ky < length // 2, ky, ky - length)))
        if LARGEST_BOUND**2 - least**2 < (half // 2) ** 2:
            thin.append(slot)
    assert thin == list(range(thin[0], thin[-1] + 1))
    return thin[0], thin[-1] + 1


def batch_order(parts):
    ring = parts // 4
    return [
        column * (parts // 2) + (place + side * (ring // 2)) * 2 + core
        for place in range(ring // 2) for column in (0, 1) for side in (0, 1) for core in (0, 1)
    ]


def build_tables(length, parts):
    cos, sin = base_tables(length)
    half, rows = length // 2, length // parts
    weight = np.where(np.arange(half) == 0, 1.0, 2.0).astype(np.float32)[:, None]
    real = np.stack([cos, -sin], axis=1)
    imag = np.stack([sin, cos], axis=1)
    inverse = np.stack([real, imag]).transpose(0, 3, 2, 1)
    turned = np.stack([np.stack([-sin, -cos], 1), np.stack([cos, -sin], 1)]).transpose(0, 3, 2, 1)
    forward = np.stack([np.stack([cos, sin], 1), np.stack([-sin, cos], 1)]).transpose(0, 3, 2, 1)
    size = 2 * length

    def slab_columns(table):
        return table.reshape(size, 2, parts, rows).transpose(0, 2, 1, 3).reshape(size, size)

    def slab_rows(table):
        return table.transpose(1, 0, 2, 3).reshape(size, size)

    kept = kept_slabs(length, parts)
    z_inv = slab_rows(inverse).reshape(parts, 2 * rows, size)[batch_order(parts)].reshape(size, size)
    y_inv = slab_columns(inverse)
    y_inv_turned = slab_columns(turned)
    y_fwd = slab_rows(forward).reshape(parts, 2 * rows, size)[kept].reshape(-1, size)
    z_fwd = slab_columns(forward)
    x_inv = np.concatenate([cos[:half] * weight, -(sin[:half] * weight)], axis=0)
    x_fwd = np.concatenate([cos[:, :half], -sin[:, :half]], axis=1)
    listed = (z_inv, y_inv, y_inv_turned, y_fwd, z_fwd, x_inv, x_fwd)
    return tuple(jnp.asarray(t.astype(np.float32)).astype(BF16) for t in listed)


def dot(a, b):
    return jnp.dot(a, b, preferred_element_type=F32)


def signed_of(index, length):
    return jnp.where(index < length // 2, index, index - length).astype(F32)


def kernel(
    parts, groups, near,
    state_in, velocity, species, table, bound, *rest,
):
    (
        *far_tables, out, kappa_out,
        state, state_sem, z_inv, y_inv, y_inv_turned, y_fwd, z_fwd, x_inv, x_fwd, table_sem, spec, work, sent, came, speeds, grads, halves, lines, flat, back_sent, back_came, stats,
        send_sem, came_sem, back_send_sem, back_sem, stat_send_sem, stat_sem, vel_sem, vel_send, vel_recv,
    ) = rest
    _, rows, length, half = state.shape
    kept = kept_slabs(length, parts)
    low = sum(1 for d in kept if d < parts // 2)
    gap = parts - len(kept)
    planes = length // parts
    pairs = planes // 2
    step_size = cfl_number * 2.0 * math.pi / length
    cell_count = float(length) ** 3
    me = lax.axis_index("fft")
    mine = lax.axis_index("scal")
    far = lax.rem(mine + groups // 2, groups)
    upper = (mine // near) * near
    up = upper + lax.rem(mine + 1, near)
    down = upper + lax.rem(mine + near - 1, near)
    far_up, far_down = lax.rem(up + groups // 2, groups), lax.rem(down + groups // 2, groups)
    across = upper + lax.rem(mine + 2, near)
    far_across = lax.rem(across + groups // 2, groups)

    table_copies = [
        pltpu.make_async_copy(src, dst, table_sem.at[k])
        for k, (src, dst) in enumerate(zip(far_tables, (z_inv, y_inv, y_inv_turned, y_fwd, z_fwd, x_inv, x_fwd)))
    ]
    state_copy = pltpu.make_async_copy(state_in, state, state_sem)
    state_copy.start()
    table_copies[0].start()
    barrier = pltpu.get_barrier_semaphore()

    @pl.loop(1, parts)
    def _(k):
        pl.semaphore_signal(barrier, inc=1, device_id={"fft": lax.rem(me + k, parts)}, device_id_type=MESH)

    for peer in (far, up, down):
        pl.semaphore_signal(barrier, inc=1, device_id={"scal": peer}, device_id_type=MESH)

    own_speeds = pltpu.make_async_copy(velocity, speeds.at[mine], vel_sem)
    own_speeds.start()
    for copy in table_copies[1:]:
        copy.start()

    kz = signed_of(lax.broadcasted_iota(jnp.int32, (length, 1), 0), length)
    kx_index = lax.broadcasted_iota(jnp.int32, (1, half), 1)
    kx = kx_index.astype(F32)
    weight = jnp.where(kx_index == 0, 1.0, 2.0).astype(F32)

    def square(row):
        ky = signed_of(me * rows + row, length)
        return kx * kx + ky * ky + kz * kz

    def put_spectrum(row, real, imag):
        here = pl.ds(pl.multiple_of(row * 2 * half, 2 * half), half)
        there = pl.ds(pl.multiple_of(row * 2 * half + half, half), half)
        spec[:length, here] = real.astype(BF16)
        spec[length:, here] = imag.astype(BF16)
        spec[:length, there] = (-kz * imag).astype(BF16)
        spec[length:, there] = (kz * real).astype(BF16)

    def fold(x):
        return jnp.sum(x.reshape(length // 8, 8, half), axis=0)

    state_copy.wait()

    @pl.loop(0, rows)
    def _(row):
        put_spectrum(row, state[0, row], state[1, row])

    table_copies[0].wait()

    def row_energy(row, total):
        real, imag = state[0, row], state[1, row]
        energy = weight * (real * real + imag * imag)
        return total[0] + fold(energy), total[1] + fold(square(row) * energy)

    batch = 8
    batches = parts // batch
    batch_rows = batch * 2 * planes
    ring = parts // 4
    my_place = lax.rem(me // 2, ring)

    def slab_at(column, place, core):
        return column * (parts // 2) + place * 2 + core

    def peer_in_batch(which, j):
        return slab_at(j // 4, which + lax.rem(j // 2, 2) * (ring // 2), lax.rem(j, 2))

    def peer_in_turn(i):
        q = i // 4
        step = jnp.where(lax.rem(q, 2) == 1, (q + 1) // 2, ring - q // 2)
        column = lax.rem(me // (parts // 2) + lax.rem(i // 2, 2), 2)
        return slab_at(column, lax.rem(my_place + step, ring), lax.rem(me + i, 2))

    def came_copy(turn, chunk, peer):
        return pltpu.make_async_remote_copy(
            src_ref=sent.at[peer, pl.ds(2 * chunk, 2)],
            dst_ref=came.at[pl.ds(2 * chunk, 2), me],
            send_sem=send_sem.at[turn],
            recv_sem=came_sem.at[turn * pairs + chunk],
            device_id={"fft": peer},
            device_id_type=MESH,
        )

    def send_planes(turn):
        def one_batch(k, _):
            which = lax.rem(my_place + k, batches)
            at = pl.multiple_of(which * batch_rows, batch_rows)
            work[...] = dot(z_inv[pl.ds(at, batch_rows), :], spec[...])
            for j in range(batch):
                peer = peer_in_batch(which, j)
                strip = work[j * 2 * planes : (j + 1) * 2 * planes, :]
                block = jnp.stack([strip[:, row * 2 * half : (row + 1) * 2 * half] for row in range(rows)])
                turned = jnp.swapaxes(block, 0, 1).reshape(planes, 2 * rows, 2 * half).astype(BF16)
                sent[peer] = turned

            if turn == 0:
                @pl.when(k == 0)
                def _():
                    pl.semaphore_wait(barrier, parts - 1 + 3)
                    speeds_copy(0, mine, far).start()
                    speeds_copy(1, mine, up).start()
                    speeds_copy(3, mine, down).start()

            @pl.loop(0, batch)
            def _(j):
                peer = peer_in_batch(which, j)

                @pl.when(peer != me)
                def _():
                    came_copy(turn, 0, peer).start()

            return 0

        lax.fori_loop(0, parts // batch, one_batch, 0)
        came[:, pl.ds(me, 1)] = sent[me][:, None]

        @pl.loop(1, pairs)
        def _(chunk):
            @pl.loop(1, parts)
            def _(i):
                came_copy(turn, chunk, peer_in_turn(parts - i)).start()

    def wait_planes(turn, chunk):
        piece = sent.at[pl.ds(0, parts - 1), pl.ds(0, 2)]
        pltpu.make_async_remote_copy(
            src_ref=piece, dst_ref=piece, send_sem=send_sem.at[turn],
            recv_sem=came_sem.at[turn * pairs + chunk], device_id={"fft": me}, device_id_type=MESH,
        ).wait_recv()

    def wait_sent(turn):
        piece = sent.at[pl.ds(0, parts - 1)]
        pltpu.make_async_remote_copy(
            src_ref=piece, dst_ref=piece, send_sem=send_sem.at[turn],
            recv_sem=came_sem.at[turn * pairs], device_id={"fft": me}, device_id_type=MESH,
        ).wait_send()

    ky_row = lax.broadcasted_iota(jnp.int32, (2 * length, 1), 0)
    ky_row = signed_of((ky_row // (2 * rows)) * rows + lax.rem(ky_row, rows), length).astype(BF16)
    kx_low = kx.astype(BF16)

    def gradient_pair(chunk):
        scaled, last = [], []
        for side in (0, 1):
            both = came[2 * chunk + side].reshape(2 * length, 2 * half)
            whole = both[:, :half]
            last.append(both[:, half:])
            scaled += [whole * kx_low, whole * ky_row]

        def put(done, column, at):
            here = slice(column * half, (column + 1) * half)
            halves[at * length : (at + 1) * length, :half] = done[:length, here].astype(BF16)
            halves[at * length : (at + 1) * length, half:] = done[length:, here].astype(BF16)

        done = dot(y_inv_turned[...], jnp.concatenate(scaled, axis=1))
        for side in (0, 1):
            for field in (0, 1):
                put(done, 2 * side + field, 2 * field + side)
        done = dot(y_inv[...], jnp.concatenate(last, axis=1))
        for side in (0, 1):
            put(done, side, 4 + side)
        grads[chunk] = dot(halves[...], x_inv[...]).reshape(6, length, length)

    def peak_of(chunk, peak):
        for side in (0, 1):
            gx, gy, gz = (grads[chunk, 2 * field + side] for field in range(3))
            size = gx * gx + gy * gy + gz * gz
            peak = jnp.maximum(peak, jnp.max(size.reshape(-1, 8, length), axis=0))
        return peak

    def forward_pair(chunk):
        terms = []
        for side in (0, 1):
            plane = 2 * chunk + side
            total = speeds[:, 0, plane].reshape(length, length).astype(F32) * grads[chunk, side]
            total = total + speeds[:, 1, plane].reshape(length, length).astype(F32) * grads[chunk, 2 + side]
            total = total + speeds[:, 2, plane].reshape(length, length).astype(F32) * grads[chunk, 4 + side]
            terms.append(total.astype(BF16))
        part = dot(jnp.concatenate(terms, axis=0), x_fwd[...]).astype(BF16)
        for side in (0, 1):
            here, lanes = slice(side * length, (side + 1) * length), slice(side * half, (side + 1) * half)
            lines[:length, lanes] = part[here, :half]
            lines[length:, lanes] = part[here, half:]
        done = dot(y_fwd[...], lines[...])
        flat[2 * chunk] = done[:, :half]
        flat[2 * chunk + 1] = done[:, half:]

    quads = rows // 4
    keeps = jnp.logical_or(me < low, me >= low + gap)
    my_slot = jnp.where(me < low, me, me - gap)
    thin_low, thin_high = narrow_slots(length, parts, half)
    my_thin = jnp.logical_and(keeps, jnp.logical_and(my_slot >= thin_low, my_slot < thin_high))
    my_wide = jnp.logical_and(keeps, jnp.logical_not(my_thin))
    lane = lax.broadcasted_iota(jnp.int32, (1, half), 1)

    def back_copy(turn, quad, slot, peer, tiles):
        return pltpu.make_async_remote_copy(
            src_ref=back_sent.at[quad, slot, pl.ds(0, tiles)], dst_ref=back_came.at[quad, me, pl.ds(0, tiles)],
            send_sem=back_send_sem.at[turn], recv_sem=back_sem.at[quads * turn + quad],
            device_id={"fft": peer}, device_id_type=MESH,
        )

    def turn_lanes(x, amount):
        return pltpu.roll(x, amount, x.ndim - 1)

    def packed(block):
        a, b, c, d = (block[k] for k in range(4))
        left = lane < half // 2
        ends = jnp.where(
            left,
            jnp.where(lane < half // 4, turn_lanes(a, half // 2), turn_lanes(b, 3 * half // 4)),
            jnp.where(lane < 3 * half // 4, c, turn_lanes(d, half // 4)),
        )
        return jnp.stack(
            [
                jnp.where(left, a, turn_lanes(b, half // 2)),
                jnp.where(left, c, turn_lanes(d, half // 2)),
                ends,
            ]
        )

    def unpacked(quad):
        first, second, ends = (
            back_came[quad, :, k].reshape(2 * length, half) for k in range(3)
        )
        left = lane < half // 2
        return (
            jnp.where(left, first, turn_lanes(ends, half // 2)),
            jnp.where(left, turn_lanes(first, half // 2), turn_lanes(ends, half // 4)),
            jnp.where(left, second, ends),
            jnp.where(left, turn_lanes(second, half // 2), turn_lanes(ends, 3 * half // 4)),
        )

    thin_count = thin_high - thin_low
    wide_count = len(kept) - thin_count

    def start_rows(turn, quad):
        @pl.loop(1, parts)
        def _(i):
            peer = peer_in_turn(parts - i)
            slot = jnp.where(peer < low, peer, peer - gap)
            wanted = jnp.logical_or(peer < low, peer >= low + gap)
            thin = jnp.logical_and(slot >= thin_low, slot < thin_high)

            @pl.when(jnp.logical_and(wanted, thin))
            def _():
                back_copy(turn, quad, slot, peer, 2).start()

            @pl.when(jnp.logical_and(wanted, jnp.logical_not(thin)))
            def _():
                back_copy(turn, quad, slot, peer, 3).start()

    def send_rows(turn):
        @pl.loop(0, quads)
        def _(quad):
            for slot in range(len(kept)):
                start = pl.multiple_of(slot * 2 * rows + quad * 8, 8)
                block = jnp.swapaxes(flat[:, pl.ds(start, 8), :], 0, 1).reshape(4, 2 * planes, half)
                back_sent[quad, slot] = packed(block).astype(BF16)
            start_rows(turn, quad)

            @pl.when(keeps)
            def _():
                back_came[quad, me] = back_sent[quad, my_slot]

    def wait_rows_sent(turn):
        for quad in range(quads):
            for tiles, count, own in ((2, thin_count, my_thin), (3, wide_count, my_wide)):
                @pl.when(own)
                def _():
                    sent_tiles(turn, tiles, count - 1).wait_send()

                @pl.when(jnp.logical_not(own))
                def _():
                    sent_tiles(turn, tiles, count).wait_send()

    def sent_tiles(turn, tiles, count):
        piece = back_sent.at[0, pl.ds(0, count), pl.ds(0, tiles)]
        return pltpu.make_async_remote_copy(
            src_ref=piece, dst_ref=piece, send_sem=back_send_sem.at[turn],
            recv_sem=back_sem.at[quads * turn], device_id={"fft": me}, device_id_type=MESH,
        )

    def wait_rows(turn, quad):
        for tiles, own in ((2, my_thin), (3, my_wide)):
            @pl.when(own)
            def _():
                piece = back_came.at[0, pl.ds(0, parts - 1), pl.ds(0, tiles)]
                pltpu.make_async_remote_copy(
                    src_ref=piece, dst_ref=piece, send_sem=back_send_sem.at[turn],
                    recv_sem=back_sem.at[quads * turn + quad], device_id={"fft": me}, device_id_type=MESH,
                ).wait_recv()

    def tendency(quad, use):
        held = unpacked(quad)
        for pair in (0, 1):
            done = dot(z_fwd[...], jnp.concatenate(held[2 * pair : 2 * pair + 2], axis=1))
            for side in (0, 1):
                use(4 * quad + 2 * pair + side, done[:, side * half : (side + 1) * half])

    def speeds_copy(k, block, peer, at=None):
        ref = speeds.at[block] if at is None else speeds.at[block, :, pl.ds(at, planes // 2)]
        return pltpu.make_async_remote_copy(
            src_ref=ref, dst_ref=ref, send_sem=vel_send.at[k], recv_sem=vel_recv.at[k],
            device_id={"scal": peer}, device_id_type=MESH,
        )

    @pl.when(jnp.logical_not(my_wide))
    def _():
        back_came[...] = jnp.zeros_like(back_came)

    own_speeds.wait()
    send_planes(0)
    zero = jnp.zeros((8, half), F32)
    variance_part, grad_part = lax.fori_loop(0, rows, row_energy, (zero, zero))
    for copy in table_copies[1:]:
        copy.wait()
    cut = planes // 2
    speeds_copy(1, down, up).wait_recv()
    speeds_copy(5, down, up, 0).start()
    speeds_copy(3, up, down).wait_recv()
    speeds_copy(7, up, down, cut).start()
    speeds_copy(0, far, far).wait_recv()
    speeds_copy(2, far, up).start()
    speeds_copy(4, far, down).start()

    def half_one(chunk, peak):
        wait_planes(0, chunk)
        gradient_pair(chunk)
        return peak_of(chunk, peak)

    peak = jnp.zeros((8, length), F32)
    peak = lax.fori_loop(0, pairs // 2, half_one, peak)
    speeds_copy(2, far_down, up).wait_recv()
    speeds_copy(6, far_down, up, 0).start()
    speeds_copy(4, far_up, down).wait_recv()
    speeds_copy(8, far_up, down, cut).start()

    def half_two(chunk, peak):
        peak = half_one(chunk, peak)
        late = chunk == pairs - 2

        @pl.when(late)
        def _():
            speeds_copy(0, mine, far).wait_send()
            for k, peer in ((1, up), (3, down)):
                speeds_copy(k, mine, peer).wait_send()
                speeds_copy(k + 1, far, peer).wait_send()
            speeds_copy(5, across, up, 0).wait()
            speeds_copy(6, far_across, up, 0).wait()
            speeds_copy(7, across, down, cut).wait()
            speeds_copy(8, far_across, down, cut).wait()

        @pl.loop(jnp.where(late, 0, chunk), chunk + 1)
        def _(k):
            forward_pair(k)

        return peak

    peak = lax.fori_loop(pairs // 2, pairs, half_two, peak)

    def whole(reduce, x):
        return reduce(reduce(x, axis=0, keepdims=True), axis=1, keepdims=True)

    stats[pl.ds(me, 1)] = jnp.where(
        lane == 0,
        whole(jnp.sum, variance_part),
        jnp.where(lane == 1, whole(jnp.sum, grad_part), whole(jnp.max, peak)),
    )[None]

    @pl.loop(1, parts)
    def _(k):
        pltpu.make_async_remote_copy(
            src_ref=stats.at[me], dst_ref=stats.at[me], send_sem=stat_send_sem, recv_sem=stat_sem,
            device_id={"fft": lax.rem(me + k, parts)}, device_id_type=MESH,
        ).start()

    send_rows(0)
    wait_sent(0)
    everyone = stats.at[pl.ds(0, parts - 1)]
    stat_wait = pltpu.make_async_remote_copy(
        src_ref=everyone, dst_ref=everyone, send_sem=stat_send_sem, recv_sem=stat_sem,
        device_id={"fft": me}, device_id_type=MESH,
    )
    stat_wait.wait_send()
    stat_wait.wait_recv()
    collected = stats[...].reshape(parts, half)
    sums = jnp.sum(collected, axis=0, keepdims=True)
    variance = sums[:, :1] / cell_count
    mean_grad = sums[:, 1:2] / cell_count
    largest = jnp.max(collected, axis=0, keepdims=True)[:, 2:3]
    count = table.shape[1]
    match = lax.broadcasted_iota(jnp.int32, (1, count), 1) == species[0]
    base = jnp.sum(jnp.where(match, table[...], 0.0), axis=1, keepdims=True)
    kappa = base * jnp.sqrt(largest) * jnp.sqrt(variance) / (mean_grad + 1e-06)
    kappa_out[...] = jnp.broadcast_to(kappa, kappa_out.shape)
    limit = bound[0].astype(F32)
    limit = limit * limit

    def to_middle(row, done):
        ksquare = square(row)
        keep = ksquare <= limit
        factor = jnp.exp(-kappa * ksquare * step_size)
        moved = []
        for part in (0, 1):
            start = state[part, row]
            rate = jnp.where(keep, -done[part * length : (part + 1) * length], 0.0)
            moved.append(factor * (start + step_size * rate))
            out[part, row] = factor * start + 0.5 * step_size * (factor * rate)
        put_spectrum(row, *moved)

    @pl.loop(0, quads)
    def _(quad):
        wait_rows(0, quad)
        tendency(quad, to_middle)

    send_planes(1)

    @pl.loop(0, pairs)
    def _(chunk):
        wait_planes(1, chunk)
        gradient_pair(chunk)
        forward_pair(chunk)

    wait_rows_sent(0)
    send_rows(1)
    wait_sent(1)

    def to_end(row, done):
        keep = square(row) <= limit
        for part in (0, 1):
            rate = jnp.where(keep, -done[part * length : (part + 1) * length], 0.0)
            out[part, row] = out[part, row] + 0.5 * step_size * rate

    @pl.loop(0, quads)
    def _(quad):
        wait_rows(1, quad)
        tendency(quad, to_end)


    wait_rows_sent(1)


def body(parts, groups, scalar_state, velocity, species, kappa_table, dealias_bound):
    _, _, rows, length, half = scalar_state.shape
    planes = length // parts
    kept = kept_slabs(length, parts)
    tables = build_tables(length, parts)
    near = groups // 2
    chunk_rows = velocity.shape[2]
    vmem = pl.BlockSpec(memory_space=pltpu.VMEM)
    smem = pl.BlockSpec(memory_space=pltpu.SMEM)
    hbm = pl.BlockSpec(memory_space=pl.ANY)
    DMA = pltpu.SemaphoreType.DMA
    new_state, kappa = pl.pallas_call(
        functools.partial(kernel, parts, groups, near),
        out_shape=(pltpu.VMEM((2, rows, length, half), F32), pltpu.VMEM((8, half), F32)),
        in_specs=[hbm, hbm, smem, vmem, smem] + [hbm] * len(tables),
        out_specs=(vmem, vmem),
        scratch_shapes=[
            pltpu.VMEM((2, rows, length, half), F32),
            DMA,
            *(pltpu.VMEM(t.shape, t.dtype) for t in tables),
            DMA((len(tables),)),
            pltpu.VMEM((2 * length, rows * 2 * half), BF16),
            pltpu.VMEM((16 * planes, rows * 2 * half), F32),
            pltpu.VMEM((parts, planes, 2 * rows, 2 * half), BF16),
            pltpu.VMEM((planes, parts, 2 * rows, 2 * half), BF16),
            pltpu.VMEM((groups, 3, planes, chunk_rows, length), BF16),
            pltpu.VMEM((planes // 2, 6, length, length), F32),
            pltpu.VMEM((6 * length, 2 * half), BF16),
            pltpu.VMEM((2 * length, 2 * half), BF16),
            pltpu.VMEM((planes, len(kept) * 2 * rows, half), F32),
            pltpu.VMEM((rows // 4, len(kept), 3, 2 * planes, half), BF16),
            pltpu.VMEM((rows // 4, parts, 3, 2 * planes, half), BF16),
            pltpu.VMEM((parts, 1, half), F32),
            DMA((2,)),
            DMA((planes,)),
            DMA((2,)),
            DMA((rows // 2,)),
            DMA,
            DMA,
            DMA,
            DMA((9,)),
            DMA((9,)),
        ],
        compiler_params=pltpu.CompilerParams(
            collective_id=0, has_side_effects=True, vmem_limit_bytes=60 * 1024 * 1024
        ),
    )(scalar_state[0], velocity, species, kappa_table[None, :], dealias_bound, *tables)
    return new_state[None], kappa[0, :1]


def solution(mesh):
    parts, groups = mesh.shape["fft"], mesh.shape["scal"]
    placed = (
        P("scal", None, "fft", None, None),
        P(None, "fft", "scal", None),
        P("scal"),
        P(),
        P("scal"),
    )
    return jax.shard_map(
        functools.partial(body, parts, groups),
        mesh=mesh,
        in_specs=placed,
        out_specs=(P("scal", None, "fft", None, None), P("scal")),
        check_vma=False,
    )
```

```python
import functools
import math

import jax
import jax.numpy as jnp
import numpy as np
from jax import lax
from jax.experimental import pallas as pl
from jax.experimental.pallas import tpu as pltpu
from jax.sharding import PartitionSpec as P

MESH = pl.DeviceIdType.MESH
cfl_number = 0.2
LARGEST_BOUND = 85
F32, BF16 = jnp.float32, jnp.bfloat16


def base_tables(length):
    index = np.arange(length)
    angles = (index[:, None] * index[None, :] % length).astype(np.float32) * np.float32(2.0 * math.pi / length)
    norming = np.float32(1.0 / math.sqrt(length))
    cos = (np.cos(angles).astype(np.float32) * norming).astype(np.float32)
    sin = (np.sin(angles).astype(np.float32) * norming).astype(np.float32)
    return cos, sin


def kept_slabs(length, parts):
    rows = length // parts
    signed = np.where(np.arange(length) < length // 2, np.arange(length), np.arange(length) - length)
    return [d for d in range(parts) if np.min(np.abs(signed[d * rows : (d + 1) * rows])) <= LARGEST_BOUND]


def narrow_slots(length, parts, half):
    rows = length // parts
    thin = []
    for slot, d in enumerate(kept_slabs(length, parts)):
        ky = np.arange(d * rows, (d + 1) * rows)
        least = np.min(np.abs(np.where(ky < length // 2, ky, ky - length)))
        if LARGEST_BOUND**2 - least**2 < (half // 2) ** 2:
            thin.append(slot)
    assert thin == list(range(thin[0], thin[-1] + 1))
    return thin[0], thin[-1] + 1


def batch_order(parts):
    ring = parts // 4
    return [
        column * (parts // 2) + (place + side * (ring // 2)) * 2 + core
        for place in range(ring // 2) for column in (0, 1) for side in (0, 1) for core in (0, 1)
    ]


def build_tables(length, parts):
    cos, sin = base_tables(length)
    half, rows = length // 2, length // parts
    weight = np.where(np.arange(half) == 0, 1.0, 2.0).astype(np.float32)[:, None]
    real = np.stack([cos, -sin], axis=1)
    imag = np.stack([sin, cos], axis=1)
    inverse = np.stack([real, imag]).transpose(0, 3, 2, 1)
    turned = np.stack([np.stack([-sin, -cos], 1), np.stack([cos, -sin], 1)]).transpose(0, 3, 2, 1)
    forward = np.stack([np.stack([cos, sin], 1), np.stack([-sin, cos], 1)]).transpose(0, 3, 2, 1)
    size = 2 * length

    def slab_columns(table):
        return table.reshape(size, 2, parts, rows).transpose(0, 2, 1, 3).reshape(size, size)

    def slab_rows(table):
        return table.transpose(1, 0, 2, 3).reshape(size, size)

    kept = kept_slabs(length, parts)
    z_inv = slab_rows(inverse).reshape(parts, 2 * rows, size)[batch_order(parts)].reshape(size, size)
    y_inv = slab_columns(inverse)
    y_inv_turned = slab_columns(turned)
    y_fwd = slab_rows(forward).reshape(parts, 2 * rows, size)[kept].reshape(-1, size)
    z_fwd = slab_columns(forward)
    x_inv = np.concatenate([cos[:half] * weight, -(sin[:half] * weight)], axis=0)
    x_fwd = np.concatenate([cos[:, :half], -sin[:, :half]], axis=1)
    listed = (z_inv, y_inv, y_inv_turned, y_fwd, z_fwd, x_inv, x_fwd)
    return tuple(jnp.asarray(t.astype(np.float32)).astype(BF16) for t in listed)


def dot(a, b):
    return jnp.dot(a, b, preferred_element_type=F32)


def signed_of(index, length):
    return jnp.where(index < length // 2, index, index - length).astype(F32)


def kernel(
    parts, groups, near,
    state_in, velocity, species, table, bound, *rest,
):
    (
        *far_tables, out, kappa_out,
        state, state_sem, z_inv, y_inv, y_inv_turned, y_fwd, z_fwd, x_inv, x_fwd, table_sem, spec, work, sent, came, speeds, grads, halves, lines, flat, back_sent, back_came, stats,
        send_sem, came_sem, back_send_sem, back_sem, stat_send_sem, stat_sem, vel_sem, vel_send, vel_recv,
    ) = rest
    _, rows, length, half = state.shape
    kept = kept_slabs(length, parts)
    low = sum(1 for d in kept if d < parts // 2)
    gap = parts - len(kept)
    planes = length // parts
    pairs = planes // 2
    step_size = cfl_number * 2.0 * math.pi / length
    cell_count = float(length) ** 3
    me = lax.axis_index("fft")
    mine = lax.axis_index("scal")
    far = lax.rem(mine + groups // 2, groups)
    upper = (mine // near) * near
    up = upper + lax.rem(mine + 1, near)
    down = upper + lax.rem(mine + near - 1, near)
    far_up, far_down = lax.rem(up + groups // 2, groups), lax.rem(down + groups // 2, groups)
    across = upper + lax.rem(mine + 2, near)
    far_across = lax.rem(across + groups // 2, groups)

    table_copies = [
        pltpu.make_async_copy(src, dst, table_sem.at[k])
        for k, (src, dst) in enumerate(zip(far_tables, (z_inv, y_inv, y_inv_turned, y_fwd, z_fwd, x_inv, x_fwd)))
    ]
    state_copy = pltpu.make_async_copy(state_in, state, state_sem)
    state_copy.start()
    table_copies[0].start()
    barrier = pltpu.get_barrier_semaphore()

    @pl.loop(1, parts)
    def _(k):
        pl.semaphore_signal(barrier, inc=1, device_id={"fft": lax.rem(me + k, parts)}, device_id_type=MESH)

    for peer in (far, up, down):
        pl.semaphore_signal(barrier, inc=1, device_id={"scal": peer}, device_id_type=MESH)

    own_speeds = pltpu.make_async_copy(velocity, speeds.at[mine], vel_sem)
    own_speeds.start()
    for copy in table_copies[1:]:
        copy.start()

    kz = signed_of(lax.broadcasted_iota(jnp.int32, (length, 1), 0), length)
    kx_index = lax.broadcasted_iota(jnp.int32, (1, half), 1)
    kx = kx_index.astype(F32)
    weight = jnp.where(kx_index == 0, 1.0, 2.0).astype(F32)

    def square(row):
        ky = signed_of(me * rows + row, length)
        return kx * kx + ky * ky + kz * kz

    def put_spectrum(row, real, imag):
        here = pl.ds(pl.multiple_of(row * 2 * half, 2 * half), half)
        there = pl.ds(pl.multiple_of(row * 2 * half + half, half), half)
        spec[:length, here] = real.astype(BF16)
        spec[length:, here] = imag.astype(BF16)
        spec[:length, there] = (-kz * imag).astype(BF16)
        spec[length:, there] = (kz * real).astype(BF16)

    def fold(x):
        return jnp.sum(x.reshape(length // 8, 8, half), axis=0)

    state_copy.wait()

    @pl.loop(0, rows)
    def _(row):
        put_spectrum(row, state[0, row], state[1, row])

    table_copies[0].wait()

    def row_energy(row, total):
        real, imag = state[0, row], state[1, row]
        energy = weight * (real * real + imag * imag)
        return total[0] + fold(energy), total[1] + fold(square(row) * energy)

    batch = 8
    batches = parts // batch
    batch_rows = batch * 2 * planes
    ring = parts // 4
    my_place = lax.rem(me // 2, ring)

    def slab_at(column, place, core):
        return column * (parts // 2) + place * 2 + core

    def peer_in_batch(which, j):
        return slab_at(j // 4, which + lax.rem(j // 2, 2) * (ring // 2), lax.rem(j, 2))

    def peer_in_turn(i):
        q = i // 4
        step = jnp.where(lax.rem(q, 2) == 1, (q + 1) // 2, ring - q // 2)
        column = lax.rem(me // (parts // 2) + lax.rem(i // 2, 2), 2)
        return slab_at(column, lax.rem(my_place + step, ring), lax.rem(me + i, 2))

    def came_copy(turn, chunk, peer):
        return pltpu.make_async_remote_copy(
            src_ref=sent.at[peer, pl.ds(2 * chunk, 2)],
            dst_ref=came.at[pl.ds(2 * chunk, 2), me],
            send_sem=send_sem.at[turn],
            recv_sem=came_sem.at[turn * pairs + chunk],
            device_id={"fft": peer},
            device_id_type=MESH,
        )

    def send_planes(turn):
        def one_batch(k, _):
            which = lax.rem(my_place + k, batches)
            at = pl.multiple_of(which * batch_rows, batch_rows)
            work[...] = dot(z_inv[pl.ds(at, batch_rows), :], spec[...])
            for j in range(batch):
                peer = peer_in_batch(which, j)
                strip = work[j * 2 * planes : (j + 1) * 2 * planes, :]
                block = jnp.stack([strip[:, row * 2 * half : (row + 1) * 2 * half] for row in range(rows)])
                turned = jnp.swapaxes(block, 0, 1).reshape(planes, 2 * rows, 2 * half).astype(BF16)
                sent[peer] = turned

            if turn == 0:
                @pl.when(k == 0)
                def _():
                    pl.semaphore_wait(barrier, parts - 1 + 3)
                    speeds_copy(0, mine, far).start()
                    speeds_copy(1, mine, up).start()
                    speeds_copy(3, mine, down).start()

            @pl.loop(0, batch)
            def _(j):
                peer = peer_in_batch(which, j)

                @pl.when(peer != me)
                def _():
                    came_copy(turn, 0, peer).start()

            return 0

        lax.fori_loop(0, parts // batch, one_batch, 0)
        came[:, pl.ds(me, 1)] = sent[me][:, None]

        @pl.loop(1, pairs)
        def _(chunk):
            @pl.loop(1, parts)
            def _(i):
                came_copy(turn, chunk, peer_in_turn(parts - i)).start()

    def wait_planes(turn, chunk):
        piece = sent.at[pl.ds(0, parts - 1), pl.ds(0, 2)]
        pltpu.make_async_remote_copy(
            src_ref=piece, dst_ref=piece, send_sem=send_sem.at[turn],
            recv_sem=came_sem.at[turn * pairs + chunk], device_id={"fft": me}, device_id_type=MESH,
        ).wait_recv()

    def wait_sent(turn):
        piece = sent.at[pl.ds(0, parts - 1)]
        pltpu.make_async_remote_copy(
            src_ref=piece, dst_ref=piece, send_sem=send_sem.at[turn],
            recv_sem=came_sem.at[turn * pairs], device_id={"fft": me}, device_id_type=MESH,
        ).wait_send()

    ky_row = lax.broadcasted_iota(jnp.int32, (2 * length, 1), 0)
    ky_row = signed_of((ky_row // (2 * rows)) * rows + lax.rem(ky_row, rows), length).astype(BF16)
    kx_low = kx.astype(BF16)

    def gradient_pair(chunk):
        scaled, last = [], []
        for side in (0, 1):
            both = came[2 * chunk + side].reshape(2 * length, 2 * half)
            whole = both[:, :half]
            last.append(both[:, half:])
            scaled += [whole * kx_low, whole * ky_row]

        def put(done, column, at):
            here = slice(column * half, (column + 1) * half)
            halves[at * length : (at + 1) * length, :half] = done[:length, here].astype(BF16)
            halves[at * length : (at + 1) * length, half:] = done[length:, here].astype(BF16)

        done = dot(y_inv_turned[...], jnp.concatenate(scaled, axis=1))
        for side in (0, 1):
            for field in (0, 1):
                put(done, 2 * side + field, 2 * field + side)
        done = dot(y_inv[...], jnp.concatenate(last, axis=1))
        for side in (0, 1):
            put(done, side, 4 + side)
        grads[chunk] = dot(halves[...], x_inv[...]).reshape(6, length, length)

    def peak_of(chunk, peak):
        for side in (0, 1):
            gx, gy, gz = (grads[chunk, 2 * field + side] for field in range(3))
            size = gx * gx + gy * gy + gz * gz
            peak = jnp.maximum(peak, jnp.max(size.reshape(-1, 8, length), axis=0))
        return peak

    def forward_pair(chunk):
        terms = []
        for side in (0, 1):
            plane = 2 * chunk + side
            total = speeds[:, 0, plane].reshape(length, length).astype(F32) * grads[chunk, side]
            total = total + speeds[:, 1, plane].reshape(length, length).astype(F32) * grads[chunk, 2 + side]
            total = total + speeds[:, 2, plane].reshape(length, length).astype(F32) * grads[chunk, 4 + side]
            terms.append(total.astype(BF16))
        part = dot(jnp.concatenate(terms, axis=0), x_fwd[...]).astype(BF16)
        for side in (0, 1):
            here, lanes = slice(side * length, (side + 1) * length), slice(side * half, (side + 1) * half)
            lines[:length, lanes] = part[here, :half]
            lines[length:, lanes] = part[here, half:]
        done = dot(y_fwd[...], lines[...])
        flat[2 * chunk] = done[:, :half]
        flat[2 * chunk + 1] = done[:, half:]

    quads = rows // 4
    keeps = jnp.logical_or(me < low, me >= low + gap)
    my_slot = jnp.where(me < low, me, me - gap)
    thin_low, thin_high = narrow_slots(length, parts, half)
    my_thin = jnp.logical_and(keeps, jnp.logical_and(my_slot >= thin_low, my_slot < thin_high))
    my_wide = jnp.logical_and(keeps, jnp.logical_not(my_thin))
    lane = lax.broadcasted_iota(jnp.int32, (1, half), 1)

    def back_copy(turn, quad, slot, peer, tiles):
        return pltpu.make_async_remote_copy(
            src_ref=back_sent.at[quad, slot, pl.ds(0, tiles)], dst_ref=back_came.at[quad, me, pl.ds(0, tiles)],
            send_sem=back_send_sem.at[turn], recv_sem=back_sem.at[quads * turn + quad],
            device_id={"fft": peer}, device_id_type=MESH,
        )

    def turn_lanes(x, amount):
        return pltpu.roll(x, amount, x.ndim - 1)

    def packed(block):
        a, b, c, d = (block[k] for k in range(4))
        left = lane < half // 2
        ends = jnp.where(
            left,
            jnp.where(lane < half // 4, turn_lanes(a, half // 2), turn_lanes(b, 3 * half // 4)),
            jnp.where(lane < 3 * half // 4, c, turn_lanes(d, half // 4)),
        )
        return jnp.stack(
            [
                jnp.where(left, a, turn_lanes(b, half // 2)),
                jnp.where(left, c, turn_lanes(d, half // 2)),
                ends,
            ]
        )

    def unpacked(quad):
        first, second, ends = (
            back_came[quad, :, k].reshape(2 * length, half) for k in range(3)
        )
        left = lane < half // 2
        return (
            jnp.where(left, first, turn_lanes(ends, half // 2)),
            jnp.where(left, turn_lanes(first, half // 2), turn_lanes(ends, half // 4)),
            jnp.where(left, second, ends),
            jnp.where(left, turn_lanes(second, half // 2), turn_lanes(ends, 3 * half // 4)),
        )

    thin_count = thin_high - thin_low
    wide_count = len(kept) - thin_count

    def start_rows(turn, quad):
        @pl.loop(1, parts)
        def _(i):
            peer = peer_in_turn(parts - i)
            slot = jnp.where(peer < low, peer, peer - gap)
            wanted = jnp.logical_or(peer < low, peer >= low + gap)
            thin = jnp.logical_and(slot >= thin_low, slot < thin_high)

            @pl.when(jnp.logical_and(wanted, thin))
            def _():
                back_copy(turn, quad, slot, peer, 2).start()

            @pl.when(jnp.logical_and(wanted, jnp.logical_not(thin)))
            def _():
                back_copy(turn, quad, slot, peer, 3).start()

    def send_rows(turn, after=None):
        for quad in range(quads):
            for slot in range(len(kept)):
                start = slot * 2 * rows + quad * 8
                block = jnp.swapaxes(flat[:, start : start + 8, :], 0, 1).reshape(4, 2 * planes, half)
                back_sent[quad, slot] = packed(block).astype(BF16)
            start_rows(turn, quad)
            if after is not None and quad == 0:
                after()

            @pl.when(keeps)
            def _():
                back_came[quad, me] = back_sent[quad, my_slot]

    def wait_rows_sent(turn):
        for quad in range(quads):
            for tiles, count, own in ((2, thin_count, my_thin), (3, wide_count, my_wide)):
                @pl.when(own)
                def _():
                    sent_tiles(turn, tiles, count - 1).wait_send()

                @pl.when(jnp.logical_not(own))
                def _():
                    sent_tiles(turn, tiles, count).wait_send()

    def sent_tiles(turn, tiles, count):
        piece = back_sent.at[0, pl.ds(0, count), pl.ds(0, tiles)]
        return pltpu.make_async_remote_copy(
            src_ref=piece, dst_ref=piece, send_sem=back_send_sem.at[turn],
            recv_sem=back_sem.at[quads * turn], device_id={"fft": me}, device_id_type=MESH,
        )

    def wait_rows(turn, quad):
        for tiles, own in ((2, my_thin), (3, my_wide)):
            @pl.when(own)
            def _():
                piece = back_came.at[0, pl.ds(0, parts - 1), pl.ds(0, tiles)]
                pltpu.make_async_remote_copy(
                    src_ref=piece, dst_ref=piece, send_sem=back_send_sem.at[turn],
                    recv_sem=back_sem.at[quads * turn + quad], device_id={"fft": me}, device_id_type=MESH,
                ).wait_recv()

    def tendency(quad, use):
        held = unpacked(quad)
        for pair in (0, 1):
            done = dot(z_fwd[...], jnp.concatenate(held[2 * pair : 2 * pair + 2], axis=1))
            for side in (0, 1):
                use(4 * quad + 2 * pair + side, done[:, side * half : (side + 1) * half])

    def speeds_copy(k, block, peer, at=None):
        ref = speeds.at[block] if at is None else speeds.at[block, :, pl.ds(at, planes // 2)]
        return pltpu.make_async_remote_copy(
            src_ref=ref, dst_ref=ref, send_sem=vel_send.at[k], recv_sem=vel_recv.at[k],
            device_id={"scal": peer}, device_id_type=MESH,
        )

    @pl.when(jnp.logical_not(my_wide))
    def _():
        back_came[...] = jnp.zeros_like(back_came)

    own_speeds.wait()
    send_planes(0)
    zero = jnp.zeros((8, half), F32)
    variance_part, grad_part = lax.fori_loop(0, rows, row_energy, (zero, zero))
    for copy in table_copies[1:]:
        copy.wait()
    cut = planes // 2
    speeds_copy(1, down, up).wait_recv()
    speeds_copy(5, down, up, 0).start()
    speeds_copy(3, up, down).wait_recv()
    speeds_copy(7, up, down, cut).start()
    speeds_copy(0, far, far).wait_recv()
    speeds_copy(2, far, up).start()
    speeds_copy(4, far, down).start()

    def half_one(chunk, peak):
        wait_planes(0, chunk)
        gradient_pair(chunk)
        return peak_of(chunk, peak)

    peak = jnp.zeros((8, length), F32)
    peak = lax.fori_loop(0, pairs // 2, half_one, peak)
    speeds_copy(2, far_down, up).wait_recv()
    speeds_copy(6, far_down, up, 0).start()
    speeds_copy(4, far_up, down).wait_recv()
    speeds_copy(8, far_up, down, cut).start()

    def half_two(chunk, peak):
        peak = half_one(chunk, peak)
        late = chunk == pairs - 2

        @pl.when(late)
        def _():
            speeds_copy(0, mine, far).wait_send()
            for k, peer in ((1, up), (3, down)):
                speeds_copy(k, mine, peer).wait_send()
                speeds_copy(k + 1, far, peer).wait_send()
            speeds_copy(5, across, up, 0).wait()
            speeds_copy(6, far_across, up, 0).wait()
            speeds_copy(7, across, down, cut).wait()
            speeds_copy(8, far_across, down, cut).wait()

        @pl.loop(jnp.where(late, 0, chunk), chunk + 1)
        def _(k):
            forward_pair(k)

        return peak

    peak = lax.fori_loop(pairs // 2, pairs, half_two, peak)

    def whole(reduce, x):
        return reduce(reduce(x, axis=0, keepdims=True), axis=1, keepdims=True)

    stats[pl.ds(me, 1)] = jnp.where(
        lane == 0,
        whole(jnp.sum, variance_part),
        jnp.where(lane == 1, whole(jnp.sum, grad_part), whole(jnp.max, peak)),
    )[None]

    def stats_out():
        @pl.loop(1, parts)
        def _(k):
            pltpu.make_async_remote_copy(
                src_ref=stats.at[me], dst_ref=stats.at[me], send_sem=stat_send_sem, recv_sem=stat_sem,
                device_id={"fft": lax.rem(me + k, parts)}, device_id_type=MESH,
            ).start()

    send_rows(0, stats_out)
    wait_sent(0)
    everyone = stats.at[pl.ds(0, parts - 1)]
    stat_wait = pltpu.make_async_remote_copy(
        src_ref=everyone, dst_ref=everyone, send_sem=stat_send_sem, recv_sem=stat_sem,
        device_id={"fft": me}, device_id_type=MESH,
    )
    stat_wait.wait_send()
    stat_wait.wait_recv()
    collected = stats[...].reshape(parts, half)
    sums = jnp.sum(collected, axis=0, keepdims=True)
    variance = sums[:, :1] / cell_count
    mean_grad = sums[:, 1:2] / cell_count
    largest = jnp.max(collected, axis=0, keepdims=True)[:, 2:3]
    count = table.shape[1]
    match = lax.broadcasted_iota(jnp.int32, (1, count), 1) == species[0]
    base = jnp.sum(jnp.where(match, table[...], 0.0), axis=1, keepdims=True)
    kappa = base * jnp.sqrt(largest) * jnp.sqrt(variance) / (mean_grad + 1e-06)
    kappa_out[...] = jnp.broadcast_to(kappa, kappa_out.shape)
    limit = bound[0].astype(F32)
    limit = limit * limit

    def to_middle(row, done):
        ksquare = square(row)
        keep = ksquare <= limit
        factor = jnp.exp(-kappa * ksquare * step_size)
        moved = []
        for part in (0, 1):
            start = state[part, row]
            rate = jnp.where(keep, -done[part * length : (part + 1) * length], 0.0)
            moved.append(factor * (start + step_size * rate))
            out[part, row] = factor * start + 0.5 * step_size * (factor * rate)
        put_spectrum(row, *moved)

    @pl.loop(0, quads)
    def _(quad):
        wait_rows(0, quad)
        tendency(quad, to_middle)

    send_planes(1)

    @pl.loop(0, pairs)
    def _(chunk):
        wait_planes(1, chunk)
        gradient_pair(chunk)
        forward_pair(chunk)

    wait_rows_sent(0)
    send_rows(1)
    wait_sent(1)

    def to_end(row, done):
        keep = square(row) <= limit
        for part in (0, 1):
            rate = jnp.where(keep, -done[part * length : (part + 1) * length], 0.0)
            out[part, row] = out[part, row] + 0.5 * step_size * rate

    @pl.loop(0, quads)
    def _(quad):
        wait_rows(1, quad)
        tendency(quad, to_end)


    wait_rows_sent(1)


def body(parts, groups, scalar_state, velocity, species, kappa_table, dealias_bound):
    _, _, rows, length, half = scalar_state.shape
    planes = length // parts
    kept = kept_slabs(length, parts)
    tables = build_tables(length, parts)
    near = groups // 2
    chunk_rows = velocity.shape[2]
    vmem = pl.BlockSpec(memory_space=pltpu.VMEM)
    smem = pl.BlockSpec(memory_space=pltpu.SMEM)
    hbm = pl.BlockSpec(memory_space=pl.ANY)
    DMA = pltpu.SemaphoreType.DMA
    new_state, kappa = pl.pallas_call(
        functools.partial(kernel, parts, groups, near),
        out_shape=(pltpu.VMEM((2, rows, length, half), F32), pltpu.VMEM((8, half), F32)),
        in_specs=[hbm, hbm, smem, vmem, smem] + [hbm] * len(tables),
        out_specs=(vmem, vmem),
        scratch_shapes=[
            pltpu.VMEM((2, rows, length, half), F32),
            DMA,
            *(pltpu.VMEM(t.shape, t.dtype) for t in tables),
            DMA((len(tables),)),
            pltpu.VMEM((2 * length, rows * 2 * half), BF16),
            pltpu.VMEM((16 * planes, rows * 2 * half), F32),
            pltpu.VMEM((parts, planes, 2 * rows, 2 * half), BF16),
            pltpu.VMEM((planes, parts, 2 * rows, 2 * half), BF16),
            pltpu.VMEM((groups, 3, planes, chunk_rows, length), BF16),
            pltpu.VMEM((planes // 2, 6, length, length), F32),
            pltpu.VMEM((6 * length, 2 * half), BF16),
            pltpu.VMEM((2 * length, 2 * half), BF16),
            pltpu.VMEM((planes, len(kept) * 2 * rows, half), F32),
            pltpu.VMEM((rows // 4, len(kept), 3, 2 * planes, half), BF16),
            pltpu.VMEM((rows // 4, parts, 3, 2 * planes, half), BF16),
            pltpu.VMEM((parts, 1, half), F32),
            DMA((2,)),
            DMA((planes,)),
            DMA((2,)),
            DMA((rows // 2,)),
            DMA,
            DMA,
            DMA,
            DMA((9,)),
            DMA((9,)),
        ],
        compiler_params=pltpu.CompilerParams(
            collective_id=0, has_side_effects=True, vmem_limit_bytes=60 * 1024 * 1024
        ),
    )(scalar_state[0], velocity, species, kappa_table[None, :], dealias_bound, *tables)
    return new_state[None], kappa[0, :1]


def solution(mesh):
    parts, groups = mesh.shape["fft"], mesh.shape["scal"]
    placed = (
        P("scal", None, "fft", None, None),
        P(None, "fft", "scal", None),
        P("scal"),
        P(),
        P("scal"),
    )
    return jax.shard_map(
        functools.partial(body, parts, groups),
        mesh=mesh,
        in_specs=placed,
        out_specs=(P("scal", None, "fft", None, None), P("scal")),
        check_vma=False,
    )
```

```python
import functools
import math

import jax
import jax.numpy as jnp
import numpy as np
from jax import lax
from jax.experimental import pallas as pl
from jax.experimental.pallas import tpu as pltpu
from jax.sharding import PartitionSpec as P

MESH = pl.DeviceIdType.MESH
cfl_number = 0.2
LARGEST_BOUND = 85
F32, BF16 = jnp.float32, jnp.bfloat16


def base_tables(length):
    index = np.arange(length)
    angles = (index[:, None] * index[None, :] % length).astype(np.float32) * np.float32(2.0 * math.pi / length)
    norming = np.float32(1.0 / math.sqrt(length))
    cos = (np.cos(angles).astype(np.float32) * norming).astype(np.float32)
    sin = (np.sin(angles).astype(np.float32) * norming).astype(np.float32)
    return cos, sin


def kept_slabs(length, parts):
    rows = length // parts
    signed = np.where(np.arange(length) < length // 2, np.arange(length), np.arange(length) - length)
    return [d for d in range(parts) if np.min(np.abs(signed[d * rows : (d + 1) * rows])) <= LARGEST_BOUND]


def narrow_slots(length, parts, half):
    rows = length // parts
    thin = []
    for slot, d in enumerate(kept_slabs(length, parts)):
        ky = np.arange(d * rows, (d + 1) * rows)
        least = np.min(np.abs(np.where(ky < length // 2, ky, ky - length)))
        if LARGEST_BOUND**2 - least**2 < (half // 2) ** 2:
            thin.append(slot)
    assert thin == list(range(thin[0], thin[-1] + 1))
    return thin[0], thin[-1] + 1


def batch_order(parts):
    ring = parts // 4
    return [
        column * (parts // 2) + (place + side * (ring // 2)) * 2 + core
        for place in range(ring // 2) for column in (0, 1) for side in (0, 1) for core in (0, 1)
    ]


def build_tables(length, parts):
    cos, sin = base_tables(length)
    half, rows = length // 2, length // parts
    weight = np.where(np.arange(half) == 0, 1.0, 2.0).astype(np.float32)[:, None]
    real = np.stack([cos, -sin], axis=1)
    imag = np.stack([sin, cos], axis=1)
    inverse = np.stack([real, imag]).transpose(0, 3, 2, 1)
    turned = np.stack([np.stack([-sin, -cos], 1), np.stack([cos, -sin], 1)]).transpose(0, 3, 2, 1)
    forward = np.stack([np.stack([cos, sin], 1), np.stack([-sin, cos], 1)]).transpose(0, 3, 2, 1)
    size = 2 * length

    def slab_columns(table):
        return table.reshape(size, 2, parts, rows).transpose(0, 2, 1, 3).reshape(size, size)

    def slab_rows(table):
        return table.transpose(1, 0, 2, 3).reshape(size, size)

    kept = kept_slabs(length, parts)
    z_inv = slab_rows(inverse).reshape(parts, 2 * rows, size)[batch_order(parts)].reshape(size, size)
    y_inv = slab_columns(inverse)
    y_inv_turned = slab_columns(turned)
    y_fwd = slab_rows(forward).reshape(parts, 2 * rows, size)[kept].reshape(-1, size)
    z_fwd = slab_columns(forward)
    x_inv = np.concatenate([cos[:half] * weight, -(sin[:half] * weight)], axis=0)
    x_fwd = np.concatenate([cos[:, :half], -sin[:, :half]], axis=1)
    listed = (z_inv, y_inv, y_inv_turned, y_fwd, z_fwd, x_inv, x_fwd)
    return tuple(jnp.asarray(t.astype(np.float32)).astype(BF16) for t in listed)


def dot(a, b):
    return jnp.dot(a, b, preferred_element_type=F32)


def signed_of(index, length):
    return jnp.where(index < length // 2, index, index - length).astype(F32)


def kernel(
    parts, groups, near,
    state_in, velocity, species, table, bound, *rest,
):
    (
        *far_tables, out, kappa_out,
        state, state_sem, z_inv, y_inv, y_inv_turned, y_fwd, z_fwd, x_inv, x_fwd, table_sem, spec, work, sent, came, speeds, grads, halves, lines, flat, back_sent, back_came, stats,
        send_sem, came_sem, back_send_sem, back_sem, stat_send_sem, stat_sem, vel_sem, vel_send, vel_recv,
    ) = rest
    _, rows, length, half = state.shape
    kept = kept_slabs(length, parts)
    low = sum(1 for d in kept if d < parts // 2)
    gap = parts - len(kept)
    planes = length // parts
    pairs = planes // 2
    step_size = cfl_number * 2.0 * math.pi / length
    cell_count = float(length) ** 3
    me = lax.axis_index("fft")
    mine = lax.axis_index("scal")
    far = lax.rem(mine + groups // 2, groups)
    upper = (mine // near) * near
    up = upper + lax.rem(mine + 1, near)
    down = upper + lax.rem(mine + near - 1, near)
    far_up, far_down = lax.rem(up + groups // 2, groups), lax.rem(down + groups // 2, groups)
    across = upper + lax.rem(mine + 2, near)
    far_across = lax.rem(across + groups // 2, groups)

    table_copies = [
        pltpu.make_async_copy(src, dst, table_sem.at[k])
        for k, (src, dst) in enumerate(zip(far_tables, (z_inv, y_inv, y_inv_turned, y_fwd, z_fwd, x_inv, x_fwd)))
    ]
    state_copies = [
        pltpu.make_async_copy(state_in.at[:, pl.ds(k * 4, 4)], state.at[:, pl.ds(k * 4, 4)], state_sem.at[k])
        for k in range(2)
    ]
    for copy in state_copies:
        copy.start()
    table_copies[0].start()
    barrier = pltpu.get_barrier_semaphore()

    @pl.loop(1, parts)
    def _(k):
        pl.semaphore_signal(barrier, inc=1, device_id={"fft": lax.rem(me + k, parts)}, device_id_type=MESH)

    for peer in (far, up, down):
        pl.semaphore_signal(barrier, inc=1, device_id={"scal": peer}, device_id_type=MESH)

    own_speeds = pltpu.make_async_copy(velocity, speeds.at[mine], vel_sem)
    own_speeds.start()
    for copy in table_copies[1:]:
        copy.start()

    kz = signed_of(lax.broadcasted_iota(jnp.int32, (length, 1), 0), length)
    kx_index = lax.broadcasted_iota(jnp.int32, (1, half), 1)
    kx = kx_index.astype(F32)
    weight = jnp.where(kx_index == 0, 1.0, 2.0).astype(F32)

    def square(row):
        ky = signed_of(me * rows + row, length)
        return kx * kx + ky * ky + kz * kz

    def put_spectrum(row, real, imag):
        here = pl.ds(pl.multiple_of(row * 2 * half, 2 * half), half)
        there = pl.ds(pl.multiple_of(row * 2 * half + half, half), half)
        spec[:length, here] = real.astype(BF16)
        spec[length:, here] = imag.astype(BF16)
        spec[:length, there] = (-kz * imag).astype(BF16)
        spec[length:, there] = (kz * real).astype(BF16)

    def fold(x):
        return jnp.sum(x.reshape(length // 8, 8, half), axis=0)

    for k, copy in enumerate(state_copies):
        copy.wait()

        @pl.loop(4 * k, 4 * k + 4)
        def _(row):
            put_spectrum(row, state[0, row], state[1, row])

    table_copies[0].wait()

    def row_energy(row, total):
        real, imag = state[0, row], state[1, row]
        energy = weight * (real * real + imag * imag)
        return total[0] + fold(energy), total[1] + fold(square(row) * energy)

    batch = 8
    batches = parts // batch
    batch_rows = batch * 2 * planes
    ring = parts // 4
    my_place = lax.rem(me // 2, ring)

    def slab_at(column, place, core):
        return column * (parts // 2) + place * 2 + core

    def peer_in_batch(which, j):
        return slab_at(j // 4, which + lax.rem(j // 2, 2) * (ring // 2), lax.rem(j, 2))

    def peer_in_turn(i):
        q = i // 4
        step = jnp.where(lax.rem(q, 2) == 1, (q + 1) // 2, ring - q // 2)
        column = lax.rem(me // (parts // 2) + lax.rem(i // 2, 2), 2)
        return slab_at(column, lax.rem(my_place + step, ring), lax.rem(me + i, 2))

    def came_copy(turn, chunk, peer):
        return pltpu.make_async_remote_copy(
            src_ref=sent.at[peer, pl.ds(2 * chunk, 2)],
            dst_ref=came.at[pl.ds(2 * chunk, 2), me],
            send_sem=send_sem.at[turn],
            recv_sem=came_sem.at[turn * pairs + chunk],
            device_id={"fft": peer},
            device_id_type=MESH,
        )

    def send_planes(turn):
        def one_batch(k, _):
            which = lax.rem(my_place + k, batches)
            at = pl.multiple_of(which * batch_rows, batch_rows)
            work[...] = dot(z_inv[pl.ds(at, batch_rows), :], spec[...])
            for j in range(batch):
                peer = peer_in_batch(which, j)
                strip = work[j * 2 * planes : (j + 1) * 2 * planes, :]
                block = jnp.stack([strip[:, row * 2 * half : (row + 1) * 2 * half] for row in range(rows)])
                turned = jnp.swapaxes(block, 0, 1).reshape(planes, 2 * rows, 2 * half).astype(BF16)
                sent[peer] = turned

            if turn == 0:
                @pl.when(k == 0)
                def _():
                    pl.semaphore_wait(barrier, parts - 1 + 3)
                    speeds_copy(0, mine, far).start()
                    speeds_copy(1, mine, up).start()
                    speeds_copy(3, mine, down).start()

            @pl.loop(0, batch)
            def _(j):
                peer = peer_in_batch(which, j)

                @pl.when(peer != me)
                def _():
                    came_copy(turn, 0, peer).start()

            return 0

        lax.fori_loop(0, parts // batch, one_batch, 0)

        @pl.loop(1, pairs)
        def _(chunk):
            @pl.loop(1, parts)
            def _(i):
                came_copy(turn, chunk, peer_in_turn(parts - i)).start()

        came[:, pl.ds(me, 1)] = sent[me][:, None]

    def wait_planes(turn, chunk):
        piece = sent.at[pl.ds(0, parts - 1), pl.ds(0, 2)]
        pltpu.make_async_remote_copy(
            src_ref=piece, dst_ref=piece, send_sem=send_sem.at[turn],
            recv_sem=came_sem.at[turn * pairs + chunk], device_id={"fft": me}, device_id_type=MESH,
        ).wait_recv()

    def wait_sent(turn):
        piece = sent.at[pl.ds(0, parts - 1)]
        pltpu.make_async_remote_copy(
            src_ref=piece, dst_ref=piece, send_sem=send_sem.at[turn],
            recv_sem=came_sem.at[turn * pairs], device_id={"fft": me}, device_id_type=MESH,
        ).wait_send()

    ky_row = lax.broadcasted_iota(jnp.int32, (2 * length, 1), 0)
    ky_row = signed_of((ky_row // (2 * rows)) * rows + lax.rem(ky_row, rows), length).astype(BF16)
    kx_low = kx.astype(BF16)

    def gradient_pair(chunk):
        scaled, last = [], []
        for side in (0, 1):
            both = came[2 * chunk + side].reshape(2 * length, 2 * half)
            whole = both[:, :half]
            last.append(both[:, half:])
            scaled += [whole * kx_low, whole * ky_row]

        def put(done, column, at):
            here = slice(column * half, (column + 1) * half)
            halves[at * length : (at + 1) * length, :half] = done[:length, here].astype(BF16)
            halves[at * length : (at + 1) * length, half:] = done[length:, here].astype(BF16)

        done = dot(y_inv_turned[...], jnp.concatenate(scaled, axis=1))
        for side in (0, 1):
            for field in (0, 1):
                put(done, 2 * side + field, 2 * field + side)
        done = dot(y_inv[...], jnp.concatenate(last, axis=1))
        for side in (0, 1):
            put(done, side, 4 + side)
        grads[chunk] = dot(halves[...], x_inv[...]).reshape(6, length, length)

    def peak_of(chunk, peak):
        for side in (0, 1):
            gx, gy, gz = (grads[chunk, 2 * field + side] for field in range(3))
            size = gx * gx + gy * gy + gz * gz
            peak = jnp.maximum(peak, jnp.max(size.reshape(-1, 8, length), axis=0))
        return peak

    def forward_pair(chunk):
        terms = []
        for side in (0, 1):
            plane = 2 * chunk + side
            total = speeds[:, 0, plane].reshape(length, length).astype(F32) * grads[chunk, side]
            total = total + speeds[:, 1, plane].reshape(length, length).astype(F32) * grads[chunk, 2 + side]
            total = total + speeds[:, 2, plane].reshape(length, length).astype(F32) * grads[chunk, 4 + side]
            terms.append(total.astype(BF16))
        part = dot(jnp.concatenate(terms, axis=0), x_fwd[...]).astype(BF16)
        for side in (0, 1):
            here, lanes = slice(side * length, (side + 1) * length), slice(side * half, (side + 1) * half)
            lines[:length, lanes] = part[here, :half]
            lines[length:, lanes] = part[here, half:]
        done = dot(y_fwd[...], lines[...])
        flat[2 * chunk] = done[:, :half]
        flat[2 * chunk + 1] = done[:, half:]

    quads = rows // 4
    keeps = jnp.logical_or(me < low, me >= low + gap)
    my_slot = jnp.where(me < low, me, me - gap)
    thin_low, thin_high = narrow_slots(length, parts, half)
    my_thin = jnp.logical_and(keeps, jnp.logical_and(my_slot >= thin_low, my_slot < thin_high))
    my_wide = jnp.logical_and(keeps, jnp.logical_not(my_thin))
    lane = lax.broadcasted_iota(jnp.int32, (1, half), 1)

    def back_copy(turn, quad, slot, peer, tiles):
        return pltpu.make_async_remote_copy(
            src_ref=back_sent.at[quad, slot, pl.ds(0, tiles)], dst_ref=back_came.at[quad, me, pl.ds(0, tiles)],
            send_sem=back_send_sem.at[turn], recv_sem=back_sem.at[quads * turn + quad],
            device_id={"fft": peer}, device_id_type=MESH,
        )

    def turn_lanes(x, amount):
        return pltpu.roll(x, amount, x.ndim - 1)

    def packed(block):
        a, b, c, d = (block[k] for k in range(4))
        left = lane < half // 2
        ends = jnp.where(
            left,
            jnp.where(lane < half // 4, turn_lanes(a, half // 2), turn_lanes(b, 3 * half // 4)),
            jnp.where(lane < 3 * half // 4, c, turn_lanes(d, half // 4)),
        )
        return jnp.stack(
            [
                jnp.where(left, a, turn_lanes(b, half // 2)),
                jnp.where(left, c, turn_lanes(d, half // 2)),
                ends,
            ]
        )

    def unpacked(quad):
        first, second, ends = (
            back_came[quad, :, k].reshape(2 * length, half) for k in range(3)
        )
        left = lane < half // 2
        return (
            jnp.where(left, first, turn_lanes(ends, half // 2)),
            jnp.where(left, turn_lanes(first, half // 2), turn_lanes(ends, half // 4)),
            jnp.where(left, second, ends),
            jnp.where(left, turn_lanes(second, half // 2), turn_lanes(ends, 3 * half // 4)),
        )

    thin_count = thin_high - thin_low
    wide_count = len(kept) - thin_count

    def start_rows(turn, quad):
        @pl.loop(1, parts)
        def _(i):
            peer = peer_in_turn(parts - i)
            slot = jnp.where(peer < low, peer, peer - gap)
            wanted = jnp.logical_or(peer < low, peer >= low + gap)
            thin = jnp.logical_and(slot >= thin_low, slot < thin_high)

            @pl.when(jnp.logical_and(wanted, thin))
            def _():
                back_copy(turn, quad, slot, peer, 2).start()

            @pl.when(jnp.logical_and(wanted, jnp.logical_not(thin)))
            def _():
                back_copy(turn, quad, slot, peer, 3).start()

    def send_rows(turn, after=None):
        for quad in range(quads):
            for slot in range(len(kept)):
                start = slot * 2 * rows + quad * 8
                block = jnp.swapaxes(flat[:, start : start + 8, :], 0, 1).reshape(4, 2 * planes, half)
                back_sent[quad, slot] = packed(block).astype(BF16)
            start_rows(turn, quad)
            if after is not None and quad == 0:
                after()

            @pl.when(keeps)
            def _():
                back_came[quad, me] = back_sent[quad, my_slot]

    def wait_rows_sent(turn):
        for quad in range(quads):
            for tiles, count, own in ((2, thin_count, my_thin), (3, wide_count, my_wide)):
                @pl.when(own)
                def _():
                    sent_tiles(turn, tiles, count - 1).wait_send()

                @pl.when(jnp.logical_not(own))
                def _():
                    sent_tiles(turn, tiles, count).wait_send()

    def sent_tiles(turn, tiles, count):
        piece = back_sent.at[0, pl.ds(0, count), pl.ds(0, tiles)]
        return pltpu.make_async_remote_copy(
            src_ref=piece, dst_ref=piece, send_sem=back_send_sem.at[turn],
            recv_sem=back_sem.at[quads * turn], device_id={"fft": me}, device_id_type=MESH,
        )

    def wait_rows(turn, quad):
        for tiles, own in ((2, my_thin), (3, my_wide)):
            @pl.when(own)
            def _():
                piece = back_came.at[0, pl.ds(0, parts - 1), pl.ds(0, tiles)]
                pltpu.make_async_remote_copy(
                    src_ref=piece, dst_ref=piece, send_sem=back_send_sem.at[turn],
                    recv_sem=back_sem.at[quads * turn + quad], device_id={"fft": me}, device_id_type=MESH,
                ).wait_recv()

    def tendency(quad, use):
        held = unpacked(quad)
        for pair in (0, 1):
            done = dot(z_fwd[...], jnp.concatenate(held[2 * pair : 2 * pair + 2], axis=1))
            for side in (0, 1):
                use(4 * quad + 2 * pair + side, done[:, side * half : (side + 1) * half])

    def speeds_copy(k, block, peer, at=None):
        ref = speeds.at[block] if at is None else speeds.at[block, :, pl.ds(at, planes // 2)]
        return pltpu.make_async_remote_copy(
            src_ref=ref, dst_ref=ref, send_sem=vel_send.at[k], recv_sem=vel_recv.at[k],
            device_id={"scal": peer}, device_id_type=MESH,
        )

    @pl.when(jnp.logical_not(my_wide))
    def _():
        back_came[...] = jnp.zeros_like(back_came)

    own_speeds.wait()
    send_planes(0)
    zero = jnp.zeros((8, half), F32)
    variance_part, grad_part = lax.fori_loop(0, rows, row_energy, (zero, zero))
    for copy in table_copies[1:]:
        copy.wait()
    cut = planes // 2
    speeds_copy(1, down, up).wait_recv()
    speeds_copy(5, down, up, 0).start()
    speeds_copy(3, up, down).wait_recv()
    speeds_copy(7, up, down, cut).start()
    speeds_copy(0, far, far).wait_recv()
    speeds_copy(2, far, up).start()
    speeds_copy(4, far, down).start()

    def half_one(chunk, peak):
        wait_planes(0, chunk)
        gradient_pair(chunk)
        return peak_of(chunk, peak)

    peak = jnp.zeros((8, length), F32)
    peak = lax.fori_loop(0, pairs // 2, half_one, peak)
    speeds_copy(2, far_down, up).wait_recv()
    speeds_copy(6, far_down, up, 0).start()
    speeds_copy(4, far_up, down).wait_recv()
    speeds_copy(8, far_up, down, cut).start()

    def half_two(chunk, peak):
        peak = half_one(chunk, peak)
        late = chunk == pairs - 2

        @pl.when(late)
        def _():
            speeds_copy(0, mine, far).wait_send()
            for k, peer in ((1, up), (3, down)):
                speeds_copy(k, mine, peer).wait_send()
                speeds_copy(k + 1, far, peer).wait_send()
            speeds_copy(5, across, up, 0).wait()
            speeds_copy(6, far_across, up, 0).wait()
            speeds_copy(7, across, down, cut).wait()
            speeds_copy(8, far_across, down, cut).wait()

        @pl.loop(jnp.where(late, 0, chunk), chunk + 1)
        def _(k):
            forward_pair(k)

        return peak

    peak = lax.fori_loop(pairs // 2, pairs, half_two, peak)

    def whole(reduce, x):
        return reduce(reduce(x, axis=0, keepdims=True), axis=1, keepdims=True)

    stats[pl.ds(me, 1)] = jnp.where(
        lane == 0,
        whole(jnp.sum, variance_part),
        jnp.where(lane == 1, whole(jnp.sum, grad_part), whole(jnp.max, peak)),
    )[None]

    def stats_out():
        @pl.loop(1, parts)
        def _(k):
            pltpu.make_async_remote_copy(
                src_ref=stats.at[me], dst_ref=stats.at[me], send_sem=stat_send_sem, recv_sem=stat_sem,
                device_id={"fft": lax.rem(me + k, parts)}, device_id_type=MESH,
            ).start()

    send_rows(0, stats_out)
    wait_sent(0)
    everyone = stats.at[pl.ds(0, parts - 1)]
    stat_wait = pltpu.make_async_remote_copy(
        src_ref=everyone, dst_ref=everyone, send_sem=stat_send_sem, recv_sem=stat_sem,
        device_id={"fft": me}, device_id_type=MESH,
    )
    stat_wait.wait_send()
    stat_wait.wait_recv()
    collected = stats[...].reshape(parts, half)
    sums = jnp.sum(collected, axis=0, keepdims=True)
    variance = sums[:, :1] / cell_count
    mean_grad = sums[:, 1:2] / cell_count
    largest = jnp.max(collected, axis=0, keepdims=True)[:, 2:3]
    count = table.shape[1]
    match = lax.broadcasted_iota(jnp.int32, (1, count), 1) == species[0]
    base = jnp.sum(jnp.where(match, table[...], 0.0), axis=1, keepdims=True)
    kappa = base * jnp.sqrt(largest) * jnp.sqrt(variance) / (mean_grad + 1e-06)
    kappa_out[...] = jnp.broadcast_to(kappa, kappa_out.shape)
    limit = bound[0].astype(F32)
    limit = limit * limit

    def to_middle(row, done):
        ksquare = square(row)
        keep = ksquare <= limit
        factor = jnp.exp(-kappa * ksquare * step_size)
        moved = []
        for part in (0, 1):
            start = state[part, row]
            rate = jnp.where(keep, -done[part * length : (part + 1) * length], 0.0)
            moved.append(factor * (start + step_size * rate))
            out[part, row] = factor * start + 0.5 * step_size * (factor * rate)
        put_spectrum(row, *moved)

    @pl.loop(0, quads)
    def _(quad):
        wait_rows(0, quad)
        tendency(quad, to_middle)

    send_planes(1)

    @pl.loop(0, pairs)
    def _(chunk):
        wait_planes(1, chunk)
        gradient_pair(chunk)
        forward_pair(chunk)

    wait_rows_sent(0)
    send_rows(1)
    wait_sent(1)

    def to_end(row, done):
        keep = square(row) <= limit
        for part in (0, 1):
            rate = jnp.where(keep, -done[part * length : (part + 1) * length], 0.0)
            out[part, row] = out[part, row] + 0.5 * step_size * rate

    @pl.loop(0, quads)
    def _(quad):
        wait_rows(1, quad)
        tendency(quad, to_end)


    wait_rows_sent(1)


def body(parts, groups, scalar_state, velocity, species, kappa_table, dealias_bound):
    _, _, rows, length, half = scalar_state.shape
    planes = length // parts
    kept = kept_slabs(length, parts)
    tables = build_tables(length, parts)
    near = groups // 2
    chunk_rows = velocity.shape[2]
    vmem = pl.BlockSpec(memory_space=pltpu.VMEM)
    smem = pl.BlockSpec(memory_space=pltpu.SMEM)
    hbm = pl.BlockSpec(memory_space=pl.ANY)
    DMA = pltpu.SemaphoreType.DMA
    new_state, kappa = pl.pallas_call(
        functools.partial(kernel, parts, groups, near),
        out_shape=(pltpu.VMEM((2, rows, length, half), F32), pltpu.VMEM((8, half), F32)),
        in_specs=[hbm, hbm, smem, vmem, smem] + [hbm] * len(tables),
        out_specs=(vmem, vmem),
        scratch_shapes=[
            pltpu.VMEM((2, rows, length, half), F32),
            DMA((2,)),
            *(pltpu.VMEM(t.shape, t.dtype) for t in tables),
            DMA((len(tables),)),
            pltpu.VMEM((2 * length, rows * 2 * half), BF16),
            pltpu.VMEM((16 * planes, rows * 2 * half), F32),
            pltpu.VMEM((parts, planes, 2 * rows, 2 * half), BF16),
            pltpu.VMEM((planes, parts, 2 * rows, 2 * half), BF16),
            pltpu.VMEM((groups, 3, planes, chunk_rows, length), BF16),
            pltpu.VMEM((planes // 2, 6, length, length), F32),
            pltpu.VMEM((6 * length, 2 * half), BF16),
            pltpu.VMEM((2 * length, 2 * half), BF16),
            pltpu.VMEM((planes, len(kept) * 2 * rows, half), F32),
            pltpu.VMEM((rows // 4, len(kept), 3, 2 * planes, half), BF16),
            pltpu.VMEM((rows // 4, parts, 3, 2 * planes, half), BF16),
            pltpu.VMEM((parts, 1, half), F32),
            DMA((2,)),
            DMA((planes,)),
            DMA((2,)),
            DMA((rows // 2,)),
            DMA,
            DMA,
            DMA,
            DMA((9,)),
            DMA((9,)),
        ],
        compiler_params=pltpu.CompilerParams(
            collective_id=0, has_side_effects=True, vmem_limit_bytes=60 * 1024 * 1024
        ),
    )(scalar_state[0], velocity, species, kappa_table[None, :], dealias_bound, *tables)
    return new_state[None], kappa[0, :1]


def solution(mesh):
    parts, groups = mesh.shape["fft"], mesh.shape["scal"]
    placed = (
        P("scal", None, "fft", None, None),
        P(None, "fft", "scal", None),
        P("scal"),
        P(),
        P("scal"),
    )
    return jax.shard_map(
        functools.partial(body, parts, groups),
        mesh=mesh,
        in_specs=placed,
        out_specs=(P("scal", None, "fft", None, None), P("scal")),
        check_vma=False,
    )
```
